512 devices in a mesh: depth: 32 (over y, x, core), tile: 16 (over z).
Axes of the slice: x: 4, y: 4, z: 16, core: 2. Of those that a mesh axis runs over, the one named last changes fastest.
Arguments:
- field: float32 [128, 1536, 1024], P('depth', 'tile'), may hold values from -6 to 6
Outputs:
- image: float32 [4, 1536, 1024], P(None, ('tile', 'depth'))
The draws below stay inside these ranges and needn't reach their ends.
All inputs are finite; a program needn't handle non-finite values.
Results may differ from the reference program's by a relative error of at most 0.0003.
Values sent between devices are 32-bit elements; how exact they have to be, the bound alone decides.
No kernel may reach another device: no remote copies, remote signals or barrier semaphores. Data moves between devices by JAX's collectives and lax.ppermute only.
A program may use at most 64 MiB of HBM per device.

```python
import jax
import jax.numpy as jnp
from jax import lax

ROWS = 96
COLS = 1024
NZ = 128
HEIGHT = 1536
N_TILE = 16


def level_of(key, extent, shards, least, high):
    gain, own = 1.0, jax.random.fold_in(key, 6)
    for position, shards_of in shards:
        steps = jnp.exp(jax.random.uniform(jax.random.fold_in(own, position), (shards_of,), jnp.float32, least / len(shards), high / len(shards)))
        gain = gain * jnp.repeat(steps, extent[position] // shards_of).reshape([-1 if axis == position else 1 for axis in range(len(extent))])
    return gain


def centred(rng, extent, width, limit, pieces=(), held_as=jnp.bfloat16):
    level = level_of(rng, extent, pieces, -0.22, 0.18) if pieces else 1.0
    result = jax.random.normal(rng, extent, jnp.float32) * width * level
    return jnp.minimum(jnp.maximum(result, -limit), limit).astype(held_as)


def setup_inputs(seed: int = 0) -> dict:
    key_of = jax.random.split(jax.random.key(seed), 2)
    field = centred(key_of[0], (NZ, HEIGHT, COLS), 1.0, 6.0, ((0, 32), (1, 16)), jnp.float32)
    return {"field": field}


centres = (-1.2, 0.3, 1.5)
spreads = (0.25, 0.35, 0.3)
heights = (2.0, 1.0, 3.0)
floor_density = 0.05
light_cols = 0.48
light_rows = 0.6
light_depth = 0.64

def emission(sample, slope_cols, slope_rows, slope_depth):
    density = floor_density + jnp.zeros_like(sample)
    for centre, spread, bump_height in zip(centres, spreads, heights):
        scaled = (sample - centre) / spread
        density = density + bump_height * jnp.exp(-scaled * scaled)
    facing = light_cols * slope_cols + light_rows * slope_rows + light_depth * slope_depth
    length = slope_cols * slope_cols + slope_rows * slope_rows + slope_depth * slope_depth + 1.0
    shading = 0.3 + 0.7 * jnp.abs(facing) * lax.rsqrt(length)
    colour = jnp.stack([shading * jax.nn.sigmoid(2.0 * sample), shading * jnp.exp(-sample * sample), shading * jax.nn.sigmoid(-2.0 * sample)])
    return (density, colour)

def integrate(density, colour, spacing):
    optics = spacing * density
    running = jnp.cumsum(optics, axis=0)
    before = jnp.concatenate([jnp.zeros_like(optics[:1]), running[:-1]], axis=0)
    weight = jnp.exp(-before) * -jnp.expm1(-optics)
    return (lax.optimization_barrier(jnp.sum(weight[None] * colour, axis=1)), jnp.exp(-running[-1]))

def reference(field):
    spacing = 3.0 / NZ
    height = field.shape[1]

    def one_block(block_index):
        first_row = block_index * ROWS
        has_below = (first_row > 0).astype(field.dtype)
        has_above = (first_row + ROWS < height).astype(field.dtype)
        row_below = lax.dynamic_slice_in_dim(field, jnp.maximum(first_row - 1, 0).astype(jnp.int32), 1, 1) * has_below
        middle = lax.dynamic_slice_in_dim(field, first_row.astype(jnp.int32), ROWS, 1)
        higher = lax.dynamic_slice_in_dim(field, jnp.minimum(first_row + ROWS, height - 1).astype(jnp.int32), 1, 1) * has_above
        window = jnp.concatenate([row_below, middle, higher], axis=1)
        further = jnp.concatenate([window[1:], jnp.zeros_like(window[:1])], axis=0)
        sample = 0.5 * (window + further)
        slope_depth = (further - window)[:, 1:-1]
        slope_rows = 0.5 * (sample[:, 2:] - sample[:, :-2])
        sample = sample[:, 1:-1]
        zero_col = jnp.zeros_like(sample[..., :1])
        slope_cols = 0.5 * (jnp.concatenate([sample[..., 1:], zero_col], axis=-1) - jnp.concatenate([zero_col, sample[..., :-1]], axis=-1))
        density, colour = emission(sample, slope_cols, slope_rows, slope_depth)
        colour_sum, through = integrate(density, colour, spacing)
        return jnp.concatenate([colour_sum, (1.0 - through)[None]], axis=0)
    blocks = lax.map(one_block, jnp.arange(N_TILE, dtype=jnp.int32))
    return jnp.transpose(blocks, (1, 0, 2, 3)).reshape(4, N_TILE * ROWS, field.shape[2])
```

```python
import functools
import math

import jax
import jax.numpy as jnp
from jax import lax
from jax.experimental import pallas as pl
from jax.experimental.pallas import tpu as pltpu
from jax.sharding import PartitionSpec as P

centres = (-1.2, 0.3, 1.5)
spreads = (0.25, 0.35, 0.3)
heights = (2.0, 1.0, 3.0)
floor_density = 0.05
light_cols = 0.48
light_rows = 0.6
light_depth = 0.64

LANES = 128
LOG2E = math.log2(math.e)
FIRST = 8


def sample_step(spacing, state, low, high, half, above, below, slope_cols):
    run, through, total, tilt, middle = state
    run = run - spacing * LOG2E * floor_density
    for centre, spread, bump in zip(centres, spreads, heights):
        offset = half - 0.5 * centre
        run = run - jnp.exp2(
            (offset * offset) * (-4.0 * LOG2E / (spread * spread)) + math.log2(bump * spacing * LOG2E)
        )
    now = jnp.exp2(run)
    weight = through - now
    slope_rows = below - above
    slope_depth = high - low
    facing = (0.7 * light_cols) * slope_cols + (0.7 * light_rows) * slope_rows + (0.7 * light_depth) * slope_depth
    length = slope_cols * slope_cols + slope_rows * slope_rows + slope_depth * slope_depth + 1.0
    lit = weight * (0.3 + jnp.abs(facing) * lax.rsqrt(length))
    total = total + lit
    tilt = tilt + lit * jnp.tanh(2.0 * half)
    middle = middle + lit * jnp.exp2((half * half) * (-4.0 * LOG2E))
    return run, now, total, tilt, middle


def render_kernel(spacing, own, partner, behind, edge, corner, out, buf, cols, sems):
    planes, rows, width = own.shape
    tiles = width // LANES
    core = lax.rem(lax.axis_index("depth"), 2)
    copies = []
    for tile in range(tiles):
        lanes = pl.ds(tile * LANES, LANES)
        for ref, slot, count in ((own, core * planes, planes), (partner, (1 - core) * planes, planes), (behind, 2 * planes, 1)):
            copies.append(
                pltpu.make_async_copy(
                    ref.at[:, :, lanes], buf.at[pl.ds(slot, count), tile, pl.ds(FIRST, rows), :], sems.at[len(copies)]
                )
            )
    for copy in copies:
        copy.start()
    for plane in range(2 * planes + 1):
        for tile in range(tiles):
            lanes = slice(tile * LANES, (tile + 1) * LANES)
            row = edge[plane : plane + 1, lanes] if plane < 2 * planes else corner[:, lanes]
            buf[plane, tile, FIRST - 1 : FIRST, :] = row
            buf[plane, tile, FIRST + rows : FIRST + rows + 1, :] = row
    for copy in copies:
        copy.wait()

    samples = 2 * planes
    groups = rows // 48
    lane = lax.broadcasted_iota(jnp.int32, (8, LANES), 1)
    leftmost, rightmost = lane == 0, lane == LANES - 1

    def picked(plane, tile, group, offset):
        return buf[plane, tile, pl.ds(FIRST + 48 * group + 3 * core + offset, 8, stride=6), :]

    def column_slopes(index, carry):
        group, row = index // 3, lax.rem(index, 3)
        before = [picked(0, tile, group, row) for tile in range(tiles)]
        for plane in range(samples):
            after = [picked(plane + 1, tile, group, row) for tile in range(tiles)]
            half = [0.25 * (a + b) for a, b in zip(before, after)]
            right = [pltpu.roll(h, LANES - 1, 1) for h in half]
            left = [pltpu.roll(h, 1, 1) for h in half]
            zero = jnp.zeros_like(half[0])
            for tile in range(tiles):
                upper = jnp.where(rightmost, right[tile + 1] if tile + 1 < tiles else zero, right[tile])
                lower = jnp.where(leftmost, left[tile - 1] if tile else zero, left[tile])
                cols[plane, index, pl.ds(tile * 8, 8), :] = upper - lower
            before = after
        return carry

    lax.fori_loop(0, 3 * groups, column_slopes, 0)

    def shade(index, carry):
        group, tile = index // tiles, lax.rem(index, tiles)
        low = [picked(0, tile, group, offset) for offset in range(-1, 4)]
        zero = jnp.zeros((8, LANES), jnp.float32)
        states = [(zero, zero + 1.0, zero, zero, zero)] * 3
        for plane in range(samples):
            high = [picked(plane + 1, tile, group, offset) for offset in range(-1, 4)]
            half = [0.25 * (a + b) for a, b in zip(low, high)]
            for row in range(3):
                states[row] = sample_step(
                    spacing,
                    states[row],
                    low[row + 1],
                    high[row + 1],
                    half[row + 1],
                    half[row],
                    half[row + 2],
                    cols[plane, group * 3 + row, pl.ds(tile * 8, 8), :],
                )
            low = high
        for row in range(3):
            run, through, total, tilt, middle = states[row]
            values = (0.5 * (total + tilt), middle, 0.5 * (total - tilt), through)
            for channel, value in enumerate(values):
                start = group * 768 + row * 32 + channel * 8 + tile
                out[pl.ds(start, 8, stride=96), :] = value
        return carry

    lax.fori_loop(0, groups * tiles, shade, 0)


def blend_kernel(slabs, out):
    count = slabs.shape[0] // 96
    for row in range(3):
        through = jnp.ones((8, LANES), jnp.float32)
        colour = [jnp.zeros((8, LANES), jnp.float32)] * 3
        for slab in range(count):
            base = slab * 96 + row * 32
            for channel in range(3):
                colour[channel] = colour[channel] + through * slabs[base + channel * 8 : base + channel * 8 + 8, :]
            through = through * slabs[base + 24 : base + 32, :]
        for channel, value in enumerate((*colour, 1.0 - through)):
            for tile in range(8):
                out[row, channel : channel + 1, tile * LANES : (tile + 1) * LANES] = value[tile : tile + 1, :]


def local(field):
    planes, rows, width = field.shape
    depth = lax.axis_size("depth")
    strips = lax.axis_size("tile")
    chips = depth // 2
    spacing = 3.0 / (planes * depth)
    core = lax.rem(lax.axis_index("depth"), 2)

    partner = lax.ppermute(field, "depth", [(i, i ^ 1) for i in range(depth)])
    first = field[:1]
    behind = lax.ppermute(first, "depth", [(2 * k + 2, 2 * k) for k in range(chips - 1)])
    behind_too = lax.ppermute(first, "depth", [(2 * k + 2, 2 * k + 1) for k in range(chips - 1)])
    behind = behind + behind_too

    mine = jnp.where(core == 1, field[:, rows - 1], field[:, 0])
    theirs = jnp.where(core == 1, partner[:, rows - 1], partner[:, 0])
    edge_out = jnp.where(core == 1, jnp.concatenate([theirs, mine]), jnp.concatenate([mine, theirs]))
    beside, diagonal = [], []
    for k in range(chips):
        for t in range(strips - 1):
            upper, lower = (2 * k + 1, t), (2 * k, t + 1)
            place = lambda d, s: d * strips + s
            beside += [(place(*upper), place(*lower)), (place(*lower), place(*upper))]
            if k + 1 < chips:
                diagonal += [
                    (place(upper[0] + 2, upper[1]), place(*lower)),
                    (place(lower[0] + 2, lower[1]), place(*upper)),
                ]
    edge = lax.ppermute(edge_out, ("depth", "tile"), beside)
    corner = lax.ppermute(edge_out[:1], ("depth", "tile"), diagonal)

    parts = pl.pallas_call(
        functools.partial(render_kernel, spacing),
        out_shape=jax.ShapeDtypeStruct((chips * 96, LANES), jnp.float32),
        in_specs=[pl.BlockSpec(memory_space=pltpu.HBM)] * 3 + [pl.BlockSpec(memory_space=pltpu.VMEM)] * 2,
        out_specs=pl.BlockSpec(memory_space=pltpu.VMEM),
        scratch_shapes=[
            pltpu.VMEM((2 * planes + 1, width // LANES, rows + 16, LANES), jnp.float32),
            pltpu.VMEM((2 * planes, 6, width // LANES * 8, LANES), jnp.float32),
            pltpu.SemaphoreType.DMA((3 * (width // LANES),)),
        ],
        name="render",
    )(field, partner, behind, edge, corner)
    groups = [[2 * k + c for k in range(chips)] for c in range(2)]
    slabs = lax.all_to_all(
        parts.reshape(chips, 96, LANES), "depth", split_axis=0, concat_axis=0, tiled=True, axis_index_groups=groups
    )
    image = pl.pallas_call(
        blend_kernel,
        out_shape=jax.ShapeDtypeStruct((3, 4, width), jnp.float32),
        in_specs=[pl.BlockSpec(memory_space=pltpu.VMEM)],
        out_specs=pl.BlockSpec(memory_space=pltpu.VMEM),
        name="blend",
    )(slabs.reshape(chips * 96, LANES))
    return jnp.transpose(image, (1, 0, 2))


def solution(mesh):
    return jax.shard_map(
        local,
        mesh=mesh,
        in_specs=(P("depth", "tile", None),),
        out_specs=P(None, ("tile", "depth"), None),
        check_vma=False,
    )
```

```python
import functools
import math

import jax
import jax.numpy as jnp
from jax import lax
from jax.experimental import pallas as pl
from jax.experimental.pallas import tpu as pltpu
from jax.sharding import PartitionSpec as P

centres = (-1.2, 0.3, 1.5)
spreads = (0.25, 0.35, 0.3)
heights = (2.0, 1.0, 3.0)
floor_density = 0.05
light_cols = 0.48
light_rows = 0.6
light_depth = 0.64

LANES = 128
LOG2E = math.log2(math.e)
FIRST = 8
PITCH = 112
VMEM = pl.BlockSpec(memory_space=pltpu.VMEM)


def sample_step(spacing, state, low, high, half, above, below, slope_cols):
    run, through, total, tilt, middle = state
    run = run - spacing * LOG2E * floor_density
    for centre, spread, bump in zip(centres, spreads, heights):
        offset = half - 0.5 * centre
        run = run - jnp.exp2(
            (offset * offset) * (-4.0 * LOG2E / (spread * spread)) + math.log2(bump * spacing * LOG2E)
        )
    now = jnp.exp2(run)
    weight = through - now
    slope_rows = below - above
    slope_depth = high - low
    facing = (0.7 * light_cols) * slope_cols + (0.7 * light_rows) * slope_rows + (0.7 * light_depth) * slope_depth
    length = slope_cols * slope_cols + slope_rows * slope_rows + slope_depth * slope_depth + 1.0
    lit = weight * (0.3 + jnp.abs(facing) * lax.rsqrt(length))
    total = total + lit
    tilt = tilt + lit * jnp.tanh(2.0 * half)
    middle = middle + lit * jnp.exp2((half * half) * (-4.0 * LOG2E))
    return run, now, total, tilt, middle


def finished(state):
    run, through, total, tilt, middle = state
    return 0.5 * (total + tilt), middle, 0.5 * (total - tilt), through


def lane_masks():
    lane = lax.broadcasted_iota(jnp.int32, (8, LANES), 1)
    return lane == 0, lane == LANES - 1


def tile_slopes(half):
    leftmost, rightmost = lane_masks()
    right = [pltpu.roll(h, LANES - 1, 1) for h in half]
    left = [pltpu.roll(h, 1, 1) for h in half]
    zero = jnp.zeros_like(half[0])
    slopes = []
    for tile in range(len(half)):
        upper = jnp.where(rightmost, right[tile + 1] if tile + 1 < len(half) else zero, right[tile])
        lower = jnp.where(leftmost, left[tile - 1] if tile else zero, left[tile])
        slopes.append(upper - lower)
    return slopes


def row_slopes(half):
    leftmost, rightmost = lane_masks()
    tile = lax.broadcasted_iota(jnp.int32, (8, LANES), 0)
    right = pltpu.roll(half, LANES - 1, 1)
    left = pltpu.roll(half, 1, 1)
    upper = jnp.where(rightmost, jnp.where(tile == 7, 0.0, pltpu.roll(right, 7, 0)), right)
    lower = jnp.where(leftmost, jnp.where(tile == 0, 0.0, pltpu.roll(left, 1, 0)), left)
    return upper - lower


def core_index():
    return lax.rem(lax.axis_index("depth"), 2)


def fetch_kernel(field, own, front, sems):
    copies = [
        pltpu.make_async_copy(field.at[pl.ds(0, 1)], front, sems.at[0]),
        pltpu.make_async_copy(field, own, sems.at[1]),
    ]
    for copy in copies:
        copy.start()
    for copy in copies:
        copy.wait()


def edge_kernel(own, partner, edge, first, inner):
    planes, rows, width = own.shape
    core = core_index()
    for plane in range(2 * planes):
        at_core0, at_core1 = (own, partner) if plane < planes else (partner, own)
        for tile in range(width // LANES):
            lanes = slice(tile * LANES, (tile + 1) * LANES)
            at = plane * (width // LANES) + tile
            row = jnp.where(
                core == 0, at_core0[plane % planes, 0:1, lanes], at_core1[plane % planes, rows - 1 : rows, lanes]
            )
            edge[at : at + 1, :] = row
            if plane == 0:
                first[at : at + 1, :] = row
            inner[at : at + 1, :] = jnp.where(
                core == 0, at_core0[plane % planes, 1:2, lanes], at_core1[plane % planes, rows - 2 : rows - 1, lanes]
            )


def bulk_kernel(spacing, own, partner, state_out, last, buf, cols):
    planes, rows, width = own.shape
    tiles = width // LANES
    core = core_index()
    for plane in range(planes):
        for tile in range(tiles):
            lanes = slice(tile * LANES, (tile + 1) * LANES)
            buf[core * planes + plane, tile, FIRST : FIRST + rows, :] = own[plane, :, lanes]
            buf[(1 - core) * planes + plane, tile, FIRST : FIRST + rows, :] = partner[plane, :, lanes]

    samples = 2 * planes - 1
    groups = rows // 48
    last[...] = buf[samples]

    def picked(plane, tile, group, offset):
        return buf[plane, tile, pl.ds(FIRST + 48 * group + 3 * core + offset, 8, stride=6), :]

    def column_slopes(index, carry):
        group, row = index // 3, lax.rem(index, 3)
        before = [picked(0, tile, group, row) for tile in range(tiles)]
        for plane in range(samples):
            after = [picked(plane + 1, tile, group, row) for tile in range(tiles)]
            slopes = tile_slopes([0.25 * (a + b) for a, b in zip(before, after)])
            for tile in range(tiles):
                cols[plane, index, pl.ds(tile * 8, 8), :] = slopes[tile]
            before = after
        return carry

    lax.fori_loop(0, 3 * groups, column_slopes, 0)

    def shade(index, carry):
        group, tile = index // tiles, lax.rem(index, tiles)
        low = [picked(0, tile, group, offset) for offset in range(-1, 4)]
        zero = jnp.zeros((8, LANES), jnp.float32)
        states = [(zero, zero + 1.0, zero, zero, zero)] * 3
        for plane in range(samples):
            high = [picked(plane + 1, tile, group, offset) for offset in range(-1, 4)]
            half = [0.25 * (a + b) for a, b in zip(low, high)]
            for row in range(3):
                states[row] = sample_step(
                    spacing,
                    states[row],
                    low[row + 1],
                    high[row + 1],
                    half[row + 1],
                    half[row],
                    half[row + 2],
                    cols[plane, group * 3 + row, pl.ds(tile * 8, 8), :],
                )
            low = high
        for row in range(3):
            for n, value in enumerate(states[row]):
                state_out[n, group * 3 + row, pl.ds(tile * 8, 8), :] = value
        return carry

    lax.fori_loop(0, groups * tiles, shade, 0)


def rest_kernel(spacing, state, last, behind0, behind1, edge, inner, beside, corner, out, buf, cols):
    tiles = last.shape[0]
    rows = behind0.shape[1]
    groups = rows // 48
    core = core_index()

    @pl.when(core == 0)
    def _():
        for tile in range(tiles):
            buf[tile, FIRST : FIRST + rows, :] = behind0[0, :, tile * LANES : (tile + 1) * LANES]

    @pl.when(core == 1)
    def _():
        for tile in range(tiles):
            buf[tile, FIRST : FIRST + rows, :] = behind1[0, :, tile * LANES : (tile + 1) * LANES]

    def picked(ref, tile, group, offset):
        return ref[tile, pl.ds(FIRST + 48 * group + 3 * core + offset, 8, stride=6), :]

    for index in range(3 * groups):
        group, row = divmod(index, 3)
        half = [0.25 * (picked(last, tile, group, row) + picked(buf, tile, group, row)) for tile in range(tiles)]
        for tile, slope in enumerate(tile_slopes(half)):
            cols[index, tile * 8 : tile * 8 + 8, :] = slope

    def shade(index, carry):
        group, tile = index // tiles, lax.rem(index, tiles)
        low = [picked(last, tile, group, offset) for offset in range(-1, 4)]
        high = [picked(buf, tile, group, offset) for offset in range(-1, 4)]
        half = [0.25 * (a + b) for a, b in zip(low, high)]
        for row in range(3):
            values = finished(
                sample_step(
                    spacing,
                    tuple(state[n, group * 3 + row, pl.ds(tile * 8, 8), :] for n in range(5)),
                    low[row + 1],
                    high[row + 1],
                    half[row + 1],
                    half[row],
                    half[row + 2],
                    cols[group * 3 + row, pl.ds(tile * 8, 8), :],
                )
            )
            for channel, value in enumerate(values):
                out[pl.ds(group * 768 + row * 32 + channel * 8 + tile, 8, stride=96), :] = value
        return carry

    lax.fori_loop(0, groups * tiles, shade, 0)

    samples = edge.shape[0] // 8

    def stacked(offset):
        view = buf.reshape(tiles * PITCH, LANES)
        return view[pl.ds(FIRST + offset, 8, stride=PITCH), :]

    def plane_rows(plane):
        at = slice(plane * 8, plane * 8 + 8)
        if plane < samples:
            return edge[at, :], inner[at, :], beside[at, :]
        return stacked((rows - 1) * core), stacked(1 + (rows - 3) * core), corner[...]

    zero = jnp.zeros((8, LANES), jnp.float32)
    line = (zero, zero + 1.0, zero, zero, zero)
    low = plane_rows(0)
    for plane in range(samples):
        high = plane_rows(plane + 1)
        half, within, beyond = [0.25 * (a + b) for a, b in zip(low, high)]
        above = jnp.where(core == 0, beyond, within)
        below = jnp.where(core == 0, within, beyond)
        line = sample_step(spacing, line, low[0], high[0], half, above, below, row_slopes(half))
        low = high
    place = core * (out.shape[0] - 32)
    for channel, value in enumerate(finished(line)):
        out[pl.ds(pl.multiple_of(place + channel * 8, 8), 8), :] = value


def blend_kernel(slabs, out):
    count = slabs.shape[0] // 96
    for row in range(3):
        through = jnp.ones((8, LANES), jnp.float32)
        colour = [jnp.zeros((8, LANES), jnp.float32)] * 3
        for slab in range(count):
            base = slab * 96 + row * 32
            for channel in range(3):
                colour[channel] = colour[channel] + through * slabs[base + channel * 8 : base + channel * 8 + 8, :]
            through = through * slabs[base + 24 : base + 32, :]
        for channel, value in enumerate((*colour, 1.0 - through)):
            for tile in range(8):
                out[row, channel : channel + 1, tile * LANES : (tile + 1) * LANES] = value[tile : tile + 1, :]


def f32(*shape):
    return jax.ShapeDtypeStruct(shape, jnp.float32)


def cost(flops, size):
    return pl.CostEstimate(flops=flops, bytes_accessed=size, transcendentals=0)


def local(field):
    planes, rows, width = field.shape
    depth = lax.axis_size("depth")
    strips = lax.axis_size("tile")
    chips = depth // 2
    tiles = width // LANES
    spacing = 3.0 / (planes * depth)

    partner = lax.ppermute(field, "depth", [(i, i ^ 1) for i in range(depth)])
    own, front = pl.pallas_call(
        fetch_kernel,
        out_shape=(f32(*field.shape), f32(1, rows, width)),
        in_specs=[pl.BlockSpec(memory_space=pltpu.HBM)],
        out_specs=(VMEM, VMEM),
        scratch_shapes=[pltpu.SemaphoreType.DMA((2,))],
        compiler_params=pltpu.CompilerParams(vmem_limit_bytes=4 << 20),
        cost_estimate=cost(1 << 10, 1 << 22),
        name="fetch",
    )(field)
    behind0 = lax.ppermute(front, "depth", [(2 * k + 2, 2 * k) for k in range(chips - 1)])
    behind1 = lax.ppermute(front, "depth", [(2 * k + 2, 2 * k + 1) for k in range(chips - 1)])

    edge, first, inner = pl.pallas_call(
        edge_kernel,
        out_shape=(f32(2 * planes * tiles, LANES), f32(tiles, LANES), f32(2 * planes * tiles, LANES)),
        in_specs=[VMEM, VMEM],
        out_specs=(VMEM, VMEM, VMEM),
        compiler_params=pltpu.CompilerParams(vmem_limit_bytes=4 << 20),
        cost_estimate=cost(1 << 20, 1 << 19),
        name="edges",
    )(own, partner)
    across, diagonal = [], []
    place = lambda d, s: d * strips + s
    for k in range(chips):
        for t in range(strips - 1):
            upper, lower = (2 * k + 1, t), (2 * k, t + 1)
            across += [(place(*upper), place(*lower)), (place(*lower), place(*upper))]
            if k + 1 < chips:
                diagonal += [
                    (place(upper[0] + 2, upper[1]), place(*lower)),
                    (place(lower[0] + 2, lower[1]), place(*upper)),
                ]
    beside = lax.ppermute(edge, ("depth", "tile"), across)
    corner = lax.ppermute(first, ("depth", "tile"), diagonal)

    state, last = pl.pallas_call(
        functools.partial(bulk_kernel, spacing),
        out_shape=(f32(5, rows // 16, tiles * 8, LANES), f32(tiles, PITCH, LANES)),
        in_specs=[VMEM, VMEM],
        out_specs=(VMEM, VMEM),
        scratch_shapes=[
            pltpu.VMEM((2 * planes, tiles, PITCH, LANES), jnp.float32),
            pltpu.VMEM((2 * planes - 1, rows // 16, tiles * 8, LANES), jnp.float32),
        ],
        compiler_params=pltpu.CompilerParams(vmem_limit_bytes=16 << 20),
        cost_estimate=cost(1 << 27, 1 << 22),
        name="bulk",
    )(own, partner)
    parts = pl.pallas_call(
        functools.partial(rest_kernel, spacing),
        out_shape=f32(chips * 96, LANES),
        in_specs=[VMEM] * 8,
        out_specs=VMEM,
        scratch_shapes=[
            pltpu.VMEM((tiles, PITCH, LANES), jnp.float32),
            pltpu.VMEM((rows // 16, tiles * 8, LANES), jnp.float32),
        ],
        compiler_params=pltpu.CompilerParams(vmem_limit_bytes=16 << 20),
        cost_estimate=cost(1 << 24, 1 << 21),
        name="rest",
    )(state, last, behind0, behind1, edge, inner, beside, corner)
    slabs = lax.all_to_all(
        parts.reshape(chips, 96, LANES),
        "depth",
        split_axis=0,
        concat_axis=0,
        tiled=True,
        axis_index_groups=[[2 * k + c for k in range(chips)] for c in range(2)],
    )
    image = pl.pallas_call(
        blend_kernel,
        out_shape=f32(3, 4, width),
        in_specs=[VMEM],
        out_specs=VMEM,
        compiler_params=pltpu.CompilerParams(vmem_limit_bytes=8 << 20),
        name="blend",
    )(slabs.reshape(chips * 96, LANES))
    return jnp.transpose(image, (1, 0, 2))


def solution(mesh):
    return jax.shard_map(
        local,
        mesh=mesh,
        in_specs=(P("depth", "tile", None),),
        out_specs=P(None, ("tile", "depth"), None),
        check_vma=False,
    )
```

```python
import functools
import math

import jax
import jax.numpy as jnp
from jax import lax
from jax.experimental import pallas as pl
from jax.experimental.pallas import tpu as pltpu
from jax.sharding import PartitionSpec as P

centres = (-1.2, 0.3, 1.5)
spreads = (0.25, 0.35, 0.3)
heights = (2.0, 1.0, 3.0)
floor_density = 0.05
light_cols = 0.48
light_rows = 0.6
light_depth = 0.64

LANES = 128
LOG2E = math.log2(math.e)
FIRST = 8
PITCH = 112
VMEM = pl.BlockSpec(memory_space=pltpu.VMEM)


def sample_step(spacing, state, low, high, half, above, below, slope_cols):
    run, through, total, tilt, middle = state
    run = run - spacing * LOG2E * floor_density
    for centre, spread, bump in zip(centres, spreads, heights):
        offset = half - 0.5 * centre
        run = run - jnp.exp2(
            (offset * offset) * (-4.0 * LOG2E / (spread * spread)) + math.log2(bump * spacing * LOG2E)
        )
    now = jnp.exp2(run)
    weight = through - now
    slope_rows = below - above
    slope_depth = high - low
    facing = (0.7 * light_cols) * slope_cols + (0.7 * light_rows) * slope_rows + (0.7 * light_depth) * slope_depth
    length = slope_cols * slope_cols + slope_rows * slope_rows + slope_depth * slope_depth + 1.0
    lit = weight * (0.3 + jnp.abs(facing) * lax.rsqrt(length))
    total = total + lit
    tilt = tilt + lit * jnp.tanh(2.0 * half)
    middle = middle + lit * jnp.exp2((half * half) * (-4.0 * LOG2E))
    return run, now, total, tilt, middle


def lane_masks():
    lane = lax.broadcasted_iota(jnp.int32, (8, LANES), 1)
    return lane == 0, lane == LANES - 1


def tile_slopes(half):
    leftmost, rightmost = lane_masks()
    right = [pltpu.roll(h, LANES - 1, 1) for h in half]
    left = [pltpu.roll(h, 1, 1) for h in half]
    zero = jnp.zeros_like(half[0])
    slopes = []
    for tile in range(len(half)):
        upper = jnp.where(rightmost, right[tile + 1] if tile + 1 < len(half) else zero, right[tile])
        lower = jnp.where(leftmost, left[tile - 1] if tile else zero, left[tile])
        slopes.append(upper - lower)
    return slopes


def row_slopes(half):
    leftmost, rightmost = lane_masks()
    tile = lax.broadcasted_iota(jnp.int32, (8, LANES), 0)
    right = pltpu.roll(half, LANES - 1, 1)
    left = pltpu.roll(half, 1, 1)
    upper = jnp.where(rightmost, jnp.where(tile == 7, 0.0, pltpu.roll(right, 7, 0)), right)
    lower = jnp.where(leftmost, jnp.where(tile == 0, 0.0, pltpu.roll(left, 1, 0)), left)
    return upper - lower


def core_index():
    return lax.rem(lax.axis_index("depth"), 2)


def outermost_kernel(field, outer):
    outer[...] = jnp.where(core_index() == 0, field[0:1], field[field.shape[0] - 1 :])


def edge_kernel(own, partner, edge, outer, inner):
    planes, rows, width = own.shape
    core = core_index()
    for plane in range(2 * planes):
        at_core0, at_core1 = (own, partner) if plane < planes else (partner, own)
        for tile in range(width // LANES):
            lanes = slice(tile * LANES, (tile + 1) * LANES)
            at = plane * (width // LANES) + tile
            row = jnp.where(
                core == 0, at_core0[plane % planes, 0:1, lanes], at_core1[plane % planes, rows - 1 : rows, lanes]
            )
            edge[at : at + 1, :] = row
            inner[at : at + 1, :] = jnp.where(
                core == 0, at_core0[plane % planes, 1:2, lanes], at_core1[plane % planes, rows - 2 : rows - 1, lanes]
            )
    tiles = width // LANES
    ends = edge[0:tiles, :], edge[(2 * planes - 1) * tiles :, :]
    outer[...] = jnp.where(core == 0, ends[1], ends[0])


def bulk_kernel(spacing, own, partner, state_out, nearest, buf, cols):
    planes, rows, width = own.shape
    tiles = width // LANES
    core = core_index()
    for plane in range(planes):
        for tile in range(tiles):
            lanes = slice(tile * LANES, (tile + 1) * LANES)
            buf[core * planes + plane, tile, FIRST : FIRST + rows, :] = own[plane, :, lanes]
            buf[(1 - core) * planes + plane, tile, FIRST : FIRST + rows, :] = partner[plane, :, lanes]

    samples = 2 * planes - 1
    groups = rows // 48
    nearest[...] = buf[samples * (1 - core)]

    def picked(plane, tile, group, offset):
        return buf[plane, tile, pl.ds(FIRST + 48 * group + 3 * core + offset, 8, stride=6), :]

    def column_slopes(index, carry):
        group, row = index // 3, lax.rem(index, 3)
        before = [picked(0, tile, group, row) for tile in range(tiles)]
        for plane in range(samples):
            after = [picked(plane + 1, tile, group, row) for tile in range(tiles)]
            slopes = tile_slopes([0.25 * (a + b) for a, b in zip(before, after)])
            for tile in range(tiles):
                cols[plane, index, pl.ds(tile * 8, 8), :] = slopes[tile]
            before = after
        return carry

    lax.fori_loop(0, 3 * groups, column_slopes, 0)

    def shade(index, carry):
        group, tile = index // tiles, lax.rem(index, tiles)
        low = [picked(0, tile, group, offset) for offset in range(-1, 4)]
        zero = jnp.zeros((8, LANES), jnp.float32)
        states = [(zero, zero + 1.0, zero, zero, zero)] * 3
        for plane in range(samples):
            high = [picked(plane + 1, tile, group, offset) for offset in range(-1, 4)]
            half = [0.25 * (a + b) for a, b in zip(low, high)]
            for row in range(3):
                states[row] = sample_step(
                    spacing,
                    states[row],
                    low[row + 1],
                    high[row + 1],
                    half[row + 1],
                    half[row],
                    half[row + 2],
                    cols[plane, group * 3 + row, pl.ds(tile * 8, 8), :],
                )
            low = high
        for row in range(3):
            for n, value in enumerate(states[row]):
                state_out[n, group * 3 + row, pl.ds(tile * 8, 8), :] = value
        return carry

    lax.fori_loop(0, groups * tiles, shade, 0)


    @pl.when(lax.axis_index("depth") == lax.axis_size("depth") - 1)
    def _():
        def slopes_at_end(index, carry):
            group, row = index // 3, lax.rem(index, 3)
            slopes = tile_slopes([0.25 * picked(samples, tile, group, row) for tile in range(tiles)])
            for tile in range(tiles):
                cols[0, index, pl.ds(tile * 8, 8), :] = slopes[tile]
            return carry

        lax.fori_loop(0, 3 * groups, slopes_at_end, 0)

        def shade_at_end(index, carry):
            group, tile = index // tiles, lax.rem(index, tiles)
            low = [picked(samples, tile, group, offset) for offset in range(-1, 4)]
            half = [0.25 * a for a in low]
            for row in range(3):
                at = (group * 3 + row, pl.ds(tile * 8, 8))
                state = sample_step(
                    spacing,
                    tuple(state_out[n, at[0], at[1], :] for n in range(5)),
                    low[row + 1],
                    jnp.zeros_like(low[0]),
                    half[row + 1],
                    half[row],
                    half[row + 2],
                    cols[0, at[0], at[1], :],
                )
                for n, value in enumerate(state):
                    state_out[n, at[0], at[1], :] = value
            return carry

        lax.fori_loop(0, groups * tiles, shade_at_end, 0)


def start_state():
    zero = jnp.zeros((8, LANES), jnp.float32)
    return zero, zero + 1.0, zero, zero, zero


def joined(core, present, bulk, outer):
    _, bulk_through, *bulk_sums = bulk
    _, outer_through, *outer_sums = outer
    outer_through = jnp.where(present, outer_through, 1.0)
    on_bulk = jnp.where(core == 0, 1.0, outer_through)
    on_outer = jnp.where(core == 0, bulk_through, jnp.where(present, 1.0, 0.0))
    total, tilt, middle = [on_bulk * a + on_outer * b for a, b in zip(bulk_sums, outer_sums)]
    return 0.5 * (total + tilt), middle, 0.5 * (total - tilt), bulk_through * outer_through


def rest_kernel(spacing, state, nearest, outer, edge, inner, beside, corner, out, buf, cols):
    tiles = nearest.shape[0]
    rows = outer.shape[1]
    groups = rows // 48
    core = core_index()
    present = lax.axis_index("depth") != 1
    for tile in range(tiles):
        buf[tile, FIRST : FIRST + rows, :] = outer[0, :, tile * LANES : (tile + 1) * LANES]
    to_high = jnp.where(core == 0, 1.0, -1.0)

    def picked(ref, tile, group, offset):
        return ref[tile, pl.ds(FIRST + 48 * group + 3 * core + offset, 8, stride=6), :]

    for index in range(3 * groups):
        group, row = divmod(index, 3)
        half = [0.25 * (picked(nearest, tile, group, row) + picked(buf, tile, group, row)) for tile in range(tiles)]
        for tile, slope in enumerate(tile_slopes(half)):
            cols[index, tile * 8 : tile * 8 + 8, :] = slope

    def shade(index, carry):
        group, tile = index // tiles, lax.rem(index, tiles)
        near = [picked(nearest, tile, group, offset) for offset in range(-1, 4)]
        far = [picked(buf, tile, group, offset) for offset in range(-1, 4)]
        half = [0.25 * (a + b) for a, b in zip(near, far)]
        for row in range(3):
            sample = sample_step(
                spacing,
                start_state(),
                to_high * near[row + 1],
                to_high * far[row + 1],
                half[row + 1],
                half[row],
                half[row + 2],
                cols[group * 3 + row, pl.ds(tile * 8, 8), :],
            )
            bulk = tuple(state[n, group * 3 + row, pl.ds(tile * 8, 8), :] for n in range(5))
            for channel, value in enumerate(joined(core, present, bulk, sample)):
                out[pl.ds(group * 768 + row * 32 + channel * 8 + tile, 8, stride=96), :] = value
        return carry

    lax.fori_loop(0, groups * tiles, shade, 0)

    planes = edge.shape[0] // 8

    def stacked(offset):
        view = buf.reshape(tiles * PITCH, LANES)
        return view[pl.ds(FIRST + offset, 8, stride=PITCH), :]

    def plane_rows(plane):
        at = slice(plane * 8, plane * 8 + 8)
        return edge[at, :], inner[at, :], beside[at, :]

    def line_step(line, low, high):
        half, within, beyond = [0.25 * (a + b) for a, b in zip(low, high)]
        above = jnp.where(core == 0, beyond, within)
        below = jnp.where(core == 0, within, beyond)
        return sample_step(spacing, line, low[0], high[0], half, above, below, row_slopes(half))

    line = start_state()
    for plane in range(planes - 1):
        line = line_step(line, plane_rows(plane), plane_rows(plane + 1))
    zero = jnp.zeros((8, LANES), jnp.float32)
    ended = line_step(line, plane_rows(planes - 1), (zero, zero, zero))
    at_end = lax.axis_index("depth") == lax.axis_size("depth") - 1
    line = tuple(jnp.where(at_end, a, b) for a, b in zip(ended, line))
    far = stacked((rows - 1) * core), stacked(1 + (rows - 3) * core), corner[...]
    near = [jnp.where(core == 0, a, b) for a, b in zip(plane_rows(planes - 1), plane_rows(0))]
    low = [jnp.where(core == 0, a, b) for a, b in zip(near, far)]
    high = [jnp.where(core == 0, b, a) for a, b in zip(near, far)]
    sample = line_step(start_state(), low, high)
    place = core * (out.shape[0] - 32)
    for channel, value in enumerate(joined(core, present, line, sample)):
        out[pl.ds(pl.multiple_of(place + channel * 8, 8), 8), :] = value


def blend_kernel(slabs, out):
    count = slabs.shape[0] // 96
    for row in range(3):
        through = jnp.ones((8, LANES), jnp.float32)
        colour = [jnp.zeros((8, LANES), jnp.float32)] * 3
        for slab in range(count):
            base = slab * 96 + row * 32
            for channel in range(3):
                colour[channel] = colour[channel] + through * slabs[base + channel * 8 : base + channel * 8 + 8, :]
            through = through * slabs[base + 24 : base + 32, :]
        for channel, value in enumerate((*colour, 1.0 - through)):
            for tile in range(8):
                out[row, channel : channel + 1, tile * LANES : (tile + 1) * LANES] = value[tile : tile + 1, :]


def f32(*shape):
    return jax.ShapeDtypeStruct(shape, jnp.float32)


def cost(flops, size):
    return pl.CostEstimate(flops=flops, bytes_accessed=size, transcendentals=0)


def local(field):
    planes, rows, width = field.shape
    depth = lax.axis_size("depth")
    strips = lax.axis_size("tile")
    chips = depth // 2
    tiles = width // LANES
    spacing = 3.0 / (planes * depth)

    partner = lax.ppermute(field, "depth", [(i, i ^ 1) for i in range(depth)])
    outer_out = pl.pallas_call(
        outermost_kernel,
        out_shape=f32(1, rows, width),
        in_specs=[VMEM],
        out_specs=VMEM,
        compiler_params=pltpu.CompilerParams(vmem_limit_bytes=4 << 20),
        cost_estimate=cost(1 << 10, 1 << 20),
        name="outermost",
    )(field)
    outer = lax.ppermute(
        outer_out,
        "depth",
        [(2 * k + 2, 2 * k) for k in range(chips - 1)] + [(2 * k + 1, 2 * k + 3) for k in range(chips - 1)],
    )

    edge, corner_out, inner = pl.pallas_call(
        edge_kernel,
        out_shape=(f32(2 * planes * tiles, LANES), f32(tiles, LANES), f32(2 * planes * tiles, LANES)),
        in_specs=[VMEM, VMEM],
        out_specs=(VMEM, VMEM, VMEM),
        compiler_params=pltpu.CompilerParams(vmem_limit_bytes=4 << 20),
        cost_estimate=cost(1 << 20, 1 << 19),
        name="edges",
    )(field, partner)
    across, diagonal = [], []
    place = lambda d, s: d * strips + s
    for k in range(chips):
        for t in range(strips - 1):
            upper, lower = (2 * k + 1, t), (2 * k, t + 1)
            across += [(place(*upper), place(*lower)), (place(*lower), place(*upper))]
            if k + 1 < chips:
                diagonal.append((place(2 * (k + 1) + 1, t), place(*lower)))
            if k:
                diagonal.append((place(2 * (k - 1), t + 1), place(*upper)))
    beside = lax.ppermute(edge, ("depth", "tile"), across)
    corner = lax.ppermute(corner_out, ("depth", "tile"), diagonal)

    state, nearest = pl.pallas_call(
        functools.partial(bulk_kernel, spacing),
        out_shape=(f32(5, rows // 16, tiles * 8, LANES), f32(tiles, PITCH, LANES)),
        in_specs=[VMEM, VMEM],
        out_specs=(VMEM, VMEM),
        scratch_shapes=[
            pltpu.VMEM((2 * planes, tiles, PITCH, LANES), jnp.float32),
            pltpu.VMEM((2 * planes - 1, rows // 16, tiles * 8, LANES), jnp.float32),
        ],
        compiler_params=pltpu.CompilerParams(vmem_limit_bytes=16 << 20),
        cost_estimate=cost(1 << 27, 1 << 22),
        name="bulk",
    )(field, partner)
    parts = pl.pallas_call(
        functools.partial(rest_kernel, spacing),
        out_shape=f32(chips * 96, LANES),
        in_specs=[VMEM] * 7,
        out_specs=VMEM,
        scratch_shapes=[
            pltpu.VMEM((tiles, PITCH, LANES), jnp.float32),
            pltpu.VMEM((rows // 16, tiles * 8, LANES), jnp.float32),
        ],
        compiler_params=pltpu.CompilerParams(vmem_limit_bytes=16 << 20),
        cost_estimate=cost(1 << 24, 1 << 21),
        name="rest",
    )(state, nearest, outer, edge, inner, beside, corner)
    slabs = lax.all_to_all(
        parts.reshape(chips, 96, LANES),
        "depth",
        split_axis=0,
        concat_axis=0,
        tiled=True,
        axis_index_groups=[[2 * k + c for k in range(chips)] for c in range(2)],
    )
    image = pl.pallas_call(
        blend_kernel,
        out_shape=f32(3, 4, width),
        in_specs=[VMEM],
        out_specs=VMEM,
        compiler_params=pltpu.CompilerParams(vmem_limit_bytes=8 << 20),
        name="blend",
    )(slabs.reshape(chips * 96, LANES))
    return jnp.transpose(image, (1, 0, 2))


def solution(mesh):
    return jax.shard_map(
        local,
        mesh=mesh,
        in_specs=(P("depth", "tile", None),),
        out_specs=P(None, ("tile", "depth"), None),
        check_vma=False,
    )
```

```python
import functools
import math

import jax
import jax.numpy as jnp
from jax import lax
from jax.experimental import pallas as pl
from jax.experimental.pallas import tpu as pltpu
from jax.sharding import PartitionSpec as P


centres = (-1.2, 0.3, 1.5)
spreads = (0.25, 0.35, 0.3)
heights = (2.0, 1.0, 3.0)
floor_density = 0.05
light_cols = 0.48
light_rows = 0.6
light_depth = 0.64

LANES = 128
LOG2E = math.log2(math.e)
FIRST = 8
PITCH = 112
VMEM = pl.BlockSpec(memory_space=pltpu.VMEM)


def sample_step(spacing, state, low, high, half, above, below, slope_cols):
    run, through, total, tilt, middle = state
    run = run - spacing * LOG2E * floor_density
    for centre, spread, bump in zip(centres, spreads, heights):
        offset = half - 0.5 * centre
        run = run - jnp.exp2(
            (offset * offset) * (-4.0 * LOG2E / (spread * spread)) + math.log2(bump * spacing * LOG2E)
        )
    now = jnp.exp2(run)
    weight = through - now
    slope_rows = below - above
    slope_depth = high - low
    facing = (0.7 * light_cols) * slope_cols + (0.7 * light_rows) * slope_rows + (0.7 * light_depth) * slope_depth
    length = slope_cols * slope_cols + slope_rows * slope_rows + slope_depth * slope_depth + 1.0
    lit = weight * (0.3 + jnp.abs(facing) * lax.rsqrt(length))
    total = total + lit
    tilt = tilt + lit * jnp.tanh(2.0 * half)
    middle = middle + lit * jnp.exp2((half * half) * (-4.0 * LOG2E))
    return run, now, total, tilt, middle


def lane_masks():
    lane = lax.broadcasted_iota(jnp.int32, (8, LANES), 1)
    return lane == 0, lane == LANES - 1


def tile_slopes(half):
    leftmost, rightmost = lane_masks()
    right = [pltpu.roll(h, LANES - 1, 1) for h in half]
    left = [pltpu.roll(h, 1, 1) for h in half]
    zero = jnp.zeros_like(half[0])
    slopes = []
    for tile in range(len(half)):
        upper = jnp.where(rightmost, right[tile + 1] if tile + 1 < len(half) else zero, right[tile])
        lower = jnp.where(leftmost, left[tile - 1] if tile else zero, left[tile])
        slopes.append(upper - lower)
    return slopes


def row_slopes(half):
    leftmost, rightmost = lane_masks()
    tile = lax.broadcasted_iota(jnp.int32, (8, LANES), 0)
    right = pltpu.roll(half, LANES - 1, 1)
    left = pltpu.roll(half, 1, 1)
    upper = jnp.where(rightmost, jnp.where(tile == 7, 0.0, pltpu.roll(right, 7, 0)), right)
    lower = jnp.where(leftmost, jnp.where(tile == 0, 0.0, pltpu.roll(left, 1, 0)), left)
    return upper - lower


def core_index():
    return lax.rem(lax.axis_index("depth"), 2)


def fetch_kernel(field, own, outer, sems):
    planes, rows, width = field.shape
    copies = [pltpu.make_async_copy(field.at[pl.ds((planes - 1) * core_index(), 1)], outer, sems.at[0])]
    for tile in range(width // LANES):
        copies.append(
            pltpu.make_async_copy(
                field.at[:, :, pl.ds(tile * LANES, LANES)],
                own.at[:, tile, pl.ds(FIRST, rows), :],
                sems.at[1 + tile],
            )
        )
    for copy in copies:
        copy.start()
    for copy in copies:
        copy.wait()


def edge_kernel(own, partner, outer, sent, edge, inner):
    planes, rows, width = partner.shape
    core = core_index()

    def row(plane, tile, n):
        lanes = slice(tile * LANES, (tile + 1) * LANES)

        def mine(slot, at):
            return own[slot, tile, FIRST + at : FIRST + at + 1, :]

        def other(slot, at):
            return partner[slot, at : at + 1, lanes]

        def beyond(slot, at):
            return outer[0, at : at + 1, lanes]

        if plane == 2 * planes:
            at_core0 = at_core1 = beyond
        else:
            at_core0, at_core1 = (mine, other) if plane < planes else (other, mine)
        return jnp.where(core == 0, at_core0(plane % planes, n), at_core1(plane % planes, rows - 1 - n))

    for plane in range(2 * planes + 1):
        for tile in range(width // LANES):
            at = plane * (width // LANES) + tile
            edge[at : at + 1, :] = row(plane, tile, 0)
            inner[at : at + 1, :] = row(plane, tile, 1)
            sent[at : at + 1, :] = row(plane, tile, rows - 1)


def start_state():
    zero = jnp.zeros((8, LANES), jnp.float32)
    return zero, zero + 1.0, zero, zero, zero


def picker(buf, core):
    def picked(plane, tile, group, offset):
        return buf[plane, tile, pl.ds(FIRST + 48 * group + 3 * core + offset, 8, stride=6), :]

    return picked


def slope_pass(picked, cols, samples, groups, tiles, ends=False):
    def step(index, carry):
        group, row = index // 3, lax.rem(index, 3)
        before = [picked(samples.start, tile, group, row) for tile in range(tiles)]
        for plane in samples:
            if ends:
                half = [0.25 * a for a in before]
            else:
                after = [picked(plane + 1, tile, group, row) for tile in range(tiles)]
                half = [0.25 * (a + b) for a, b in zip(before, after)]
                before = after
            for tile, slope in enumerate(tile_slopes(half)):
                cols[plane - samples.start, index, pl.ds(tile * 8, 8), :] = slope
        return carry

    lax.fori_loop(0, 3 * groups, step, 0)


def shade_pass(spacing, picked, cols, samples, groups, tiles, load, save, ends=False):
    def step(index, carry):
        group, tile = index // tiles, lax.rem(index, tiles)
        at = [(group * 3 + row, pl.ds(tile * 8, 8)) for row in range(3)]
        low = [picked(samples.start, tile, group, offset) for offset in range(-1, 4)]
        states = [load(*at[row]) for row in range(3)]
        for plane in samples:
            if ends:
                high = [jnp.zeros_like(low[0])] * 5
                half = [0.25 * a for a in low]
            else:
                high = [picked(plane + 1, tile, group, offset) for offset in range(-1, 4)]
                half = [0.25 * (a + b) for a, b in zip(low, high)]
            for row in range(3):
                states[row] = sample_step(
                    spacing,
                    states[row],
                    low[row + 1],
                    high[row + 1],
                    half[row + 1],
                    half[row],
                    half[row + 2],
                    cols[plane - samples.start, at[row][0], at[row][1], :],
                )
            low = high
        for row in range(3):
            save(*at[row], states[row])
        return carry

    lax.fori_loop(0, groups * tiles, step, 0)


def join(first, nearer, farther):
    near_through, *near_sums = nearer
    far_through, *far_sums = farther
    on_near = jnp.where(first, 1.0, far_through)
    on_far = jnp.where(first, near_through, 1.0)
    return (near_through * far_through, *[on_near * a + on_far * b for a, b in zip(near_sums, far_sums)])


def own_kernel(spacing, own, sums, cols):
    planes, tiles = own.shape[:2]
    groups = sums.shape[1] // 3
    picked = picker(own, core_index())

    def load(block, part):
        return tuple(sums[n, block, part, :] for n in range(5))

    def save(block, part, state):
        for n, value in enumerate(state):
            sums[n, block, part, :] = value

    inside = range(planes - 1)
    slope_pass(picked, cols, inside, groups, tiles)
    shade_pass(spacing, picked, cols, inside, groups, tiles, lambda *_: start_state(), save)

    @pl.when(lax.axis_index("depth") == lax.axis_size("depth") - 1)
    def _():
        last = range(planes - 1, planes)
        slope_pass(picked, cols, last, groups, tiles, ends=True)
        shade_pass(spacing, picked, cols, last, groups, tiles, load, save, ends=True)


def partner_kernel(spacing, own, partner, own_sums, sums, nearest, buf, cols):
    planes, rows, width = partner.shape
    tiles, groups = width // LANES, rows // 48
    core = core_index()
    for tile in range(tiles):
        lanes = slice(tile * LANES, (tile + 1) * LANES)
        for plane in range(planes):
            buf[plane + 1 - core, tile, FIRST : FIRST + rows, :] = partner[plane, :, lanes]
        buf[planes * core, tile, :, :] = jnp.where(core == 0, own[planes - 1, tile], own[0, tile])
    nearest[...] = buf[planes * (1 - core)]
    picked = picker(buf, core)

    def save(block, part, state):
        nearer = tuple(own_sums[n, block, part, :] for n in range(1, 5))
        for n, value in enumerate(join(core == 0, nearer, state[1:])):
            sums[n, block, part, :] = value

    samples = range(planes)
    slope_pass(picked, cols, samples, groups, tiles)
    shade_pass(spacing, picked, cols, samples, groups, tiles, lambda *_: start_state(), save)


def finished(core, present, bulk, outer):
    outer = (jnp.where(present, outer[0], 1.0), *[jnp.where(present, value, 0.0) for value in outer[1:]])
    through, total, tilt, middle = join(core == 0, bulk, outer)
    return 0.5 * (total + tilt), middle, 0.5 * (total - tilt), through


def outer_kernel(spacing, sums, nearest, outer, edge, inner, beside, out, buf, cols):
    tiles = nearest.shape[0]
    rows = outer.shape[1]
    groups = rows // 48
    core = core_index()
    present = lax.axis_index("depth") != 1
    for tile in range(tiles):
        buf[tile, FIRST : FIRST + rows, :] = outer[0, :, tile * LANES : (tile + 1) * LANES]
    to_high = jnp.where(core == 0, 1.0, -1.0)

    def picked(ref, tile, group, offset):
        return ref[tile, pl.ds(FIRST + 48 * group + 3 * core + offset, 8, stride=6), :]

    for index in range(3 * groups):
        group, row = divmod(index, 3)
        half = [0.25 * (picked(nearest, tile, group, row) + picked(buf, tile, group, row)) for tile in range(tiles)]
        for tile, slope in enumerate(tile_slopes(half)):
            cols[index, tile * 8 : tile * 8 + 8, :] = slope

    def shade(index, carry):
        group, tile = index // tiles, lax.rem(index, tiles)
        near = [picked(nearest, tile, group, offset) for offset in range(-1, 4)]
        far = [picked(buf, tile, group, offset) for offset in range(-1, 4)]
        half = [0.25 * (a + b) for a, b in zip(near, far)]
        for row in range(3):
            sample = sample_step(
                spacing,
                start_state(),
                to_high * near[row + 1],
                to_high * far[row + 1],
                half[row + 1],
                half[row],
                half[row + 2],
                cols[group * 3 + row, pl.ds(tile * 8, 8), :],
            )
            bulk = tuple(sums[n, group * 3 + row, pl.ds(tile * 8, 8), :] for n in range(4))
            for channel, value in enumerate(finished(core, present, bulk, sample[1:])):
                out[pl.ds(group * 768 + row * 32 + channel * 8 + tile, 8, stride=96), :] = value
        return carry

    lax.fori_loop(0, groups * tiles, shade, 0)

    planes = edge.shape[0] // 8 - 1

    def plane_rows(plane):
        at = slice(plane * 8, plane * 8 + 8)
        return edge[at, :], inner[at, :], beside[at, :]

    def line_step(line, low, high):
        half, within, beyond = [0.25 * (a + b) for a, b in zip(low, high)]
        above = jnp.where(core == 0, beyond, within)
        below = jnp.where(core == 0, within, beyond)
        return sample_step(spacing, line, low[0], high[0], half, above, below, row_slopes(half))

    line = start_state()
    for plane in range(planes - 1):
        line = line_step(line, plane_rows(plane), plane_rows(plane + 1))
    zero = jnp.zeros((8, LANES), jnp.float32)
    ended = line_step(line, plane_rows(planes - 1), (zero, zero, zero))
    at_end = lax.axis_index("depth") == lax.axis_size("depth") - 1
    line = tuple(jnp.where(at_end, a, b) for a, b in zip(ended, line))
    far = plane_rows(planes)
    near = [jnp.where(core == 0, a, b) for a, b in zip(plane_rows(planes - 1), plane_rows(0))]
    low = [jnp.where(core == 0, a, b) for a, b in zip(near, far)]
    high = [jnp.where(core == 0, b, a) for a, b in zip(near, far)]
    sample = line_step(start_state(), low, high)
    place = core * (out.shape[0] - 32)
    for channel, value in enumerate(finished(core, present, line[1:], sample[1:])):
        out[pl.ds(pl.multiple_of(place + channel * 8, 8), 8), :] = value


def blend_kernel(slabs, out):
    count = slabs.shape[0] // 96
    for row in range(3):
        through = jnp.ones((8, LANES), jnp.float32)
        colour = [jnp.zeros((8, LANES), jnp.float32)] * 3
        for slab in range(count):
            base = slab * 96 + row * 32
            for channel in range(3):
                colour[channel] = colour[channel] + through * slabs[base + channel * 8 : base + channel * 8 + 8, :]
            through = through * slabs[base + 24 : base + 32, :]
        for channel, value in enumerate((*colour, 1.0 - through)):
            for tile in range(8):
                out[row, channel : channel + 1, tile * LANES : (tile + 1) * LANES] = value[tile : tile + 1, :]


def f32(*shape):
    return jax.ShapeDtypeStruct(shape, jnp.float32)


def cost(flops, size):
    return pl.CostEstimate(flops=flops, bytes_accessed=size, transcendentals=0)


def composited(field):
    planes, rows, width = field.shape
    depth = lax.axis_size("depth")
    strips = lax.axis_size("tile")
    chips = depth // 2
    tiles = width // LANES
    spacing = 3.0 / (planes * depth)

    own, outer_out = pl.pallas_call(
        fetch_kernel,
        out_shape=(f32(planes, tiles, PITCH, LANES), f32(1, rows, width)),
        in_specs=[pl.BlockSpec(memory_space=pltpu.HBM)],
        out_specs=(VMEM, VMEM),
        scratch_shapes=[pltpu.SemaphoreType.DMA((1 + tiles,))],
        compiler_params=pltpu.CompilerParams(vmem_limit_bytes=4 << 20),
        cost_estimate=cost(1 << 10, 1 << 22),
        name="fetch",
    )(field)
    outer = lax.ppermute(
        outer_out,
        "depth",
        [(2 * k + 2, 2 * k) for k in range(chips - 1)] + [(2 * k + 1, 2 * k + 3) for k in range(chips - 1)],
    )
    partner = lax.ppermute(field, "depth", [(i, i ^ 1) for i in range(depth)])

    lines = (2 * planes + 1) * tiles
    sent, edge, inner = pl.pallas_call(
        edge_kernel,
        out_shape=(f32(lines, LANES), f32(lines, LANES), f32(lines, LANES)),
        in_specs=[VMEM, VMEM, VMEM],
        out_specs=(VMEM, VMEM, VMEM),
        compiler_params=pltpu.CompilerParams(vmem_limit_bytes=4 << 20),
        cost_estimate=cost(1 << 20, 1 << 19),
        name="edges",
    )(own, partner, outer)
    place = lambda d, s: d * strips + s
    beside = lax.ppermute(
        sent,
        ("depth", "tile"),
        [(place(2 * k, t), place(2 * k, t + 1)) for k in range(chips) for t in range(strips - 1)]
        + [(place(2 * k + 1, t + 1), place(2 * k + 1, t)) for k in range(chips) for t in range(strips - 1)],
    )

    blocks = rows // 16
    own_sums = pl.pallas_call(
        functools.partial(own_kernel, spacing),
        out_shape=f32(5, blocks, tiles * 8, LANES),
        in_specs=[VMEM],
        out_specs=VMEM,
        scratch_shapes=[
                pltpu.VMEM((planes - 1, blocks, tiles * 8, LANES), jnp.float32),
        ],
        compiler_params=pltpu.CompilerParams(vmem_limit_bytes=12 << 20),
        cost_estimate=cost(1 << 26, 1 << 21),
        name="own",
    )(own)
    sums, nearest = pl.pallas_call(
        functools.partial(partner_kernel, spacing),
        out_shape=(f32(4, blocks, tiles * 8, LANES), f32(tiles, PITCH, LANES)),
        in_specs=[VMEM] * 3,
        out_specs=(VMEM, VMEM),
        scratch_shapes=[
            pltpu.VMEM((planes + 1, tiles, PITCH, LANES), jnp.float32),
            pltpu.VMEM((planes, blocks, tiles * 8, LANES), jnp.float32),
        ],
        compiler_params=pltpu.CompilerParams(vmem_limit_bytes=12 << 20),
        cost_estimate=cost(1 << 26, 1 << 21),
        name="partner",
    )(own, partner, own_sums)
    parts = pl.pallas_call(
        functools.partial(outer_kernel, spacing),
        out_shape=f32(chips * 96, LANES),
        in_specs=[VMEM] * 6,
        out_specs=VMEM,
        scratch_shapes=[
            pltpu.VMEM((tiles, PITCH, LANES), jnp.float32),
            pltpu.VMEM((rows // 16, tiles * 8, LANES), jnp.float32),
        ],
        compiler_params=pltpu.CompilerParams(vmem_limit_bytes=16 << 20),
        cost_estimate=cost(1 << 24, 1 << 21),
        name="outer",
    )(sums, nearest, outer, edge, inner, beside)
    slabs = lax.all_to_all(
        parts.reshape(chips, 96, LANES),
        "depth",
        split_axis=0,
        concat_axis=0,
        tiled=True,
        axis_index_groups=[[2 * k + c for k in range(chips)] for c in range(2)],
    )
    image = pl.pallas_call(
        blend_kernel,
        out_shape=f32(3, 4, width),
        in_specs=[VMEM],
        out_specs=VMEM,
        compiler_params=pltpu.CompilerParams(vmem_limit_bytes=8 << 20),
        name="blend",
    )(slabs.reshape(chips * 96, LANES))
    return jnp.transpose(image, (1, 0, 2))


def solution(mesh):
    return jax.shard_map(
        composited,
        mesh=mesh,
        in_specs=(P("depth", "tile", None),),
        out_specs=P(None, ("tile", "depth"), None),
        check_vma=False,
    )
```

```python
import functools
import math

import jax
import jax.numpy as jnp
from jax import lax
from jax.experimental import pallas as pl
from jax.experimental.pallas import tpu as pltpu
from jax.sharding import PartitionSpec as P


centres = (-1.2, 0.3, 1.5)
spreads = (0.25, 0.35, 0.3)
heights = (2.0, 1.0, 3.0)
floor_density = 0.05
light_cols = 0.48
light_rows = 0.6
light_depth = 0.64

LANES = 128
LOG2E = math.log2(math.e)
FIRST = 8
PITCH = 112
VMEM = pl.BlockSpec(memory_space=pltpu.VMEM)


def sample_step(spacing, state, low, high, half, above, below, slope_cols):
    run, through, total, tilt, middle = state
    run = run - spacing * LOG2E * floor_density
    for centre, spread, bump in zip(centres, spreads, heights):
        offset = half - 0.5 * centre
        run = run - jnp.exp2(
            (offset * offset) * (-4.0 * LOG2E / (spread * spread)) + math.log2(bump * spacing * LOG2E)
        )
    now = jnp.exp2(run)
    weight = through - now
    slope_rows = below - above
    slope_depth = high - low
    facing = (0.7 * light_cols) * slope_cols + (0.7 * light_rows) * slope_rows + (0.7 * light_depth) * slope_depth
    length = slope_cols * slope_cols + slope_rows * slope_rows + slope_depth * slope_depth + 1.0
    lit = weight * (0.3 + jnp.abs(facing) * lax.rsqrt(length))
    total = total + lit
    tilt = tilt + lit * jnp.tanh(2.0 * half)
    middle = middle + lit * jnp.exp2((half * half) * (-4.0 * LOG2E))
    return run, now, total, tilt, middle


def lane_masks():
    lane = lax.broadcasted_iota(jnp.int32, (8, LANES), 1)
    return lane == 0, lane == LANES - 1


def row_slopes(half):
    leftmost, rightmost = lane_masks()
    tile = lax.broadcasted_iota(jnp.int32, (8, LANES), 0)
    right = pltpu.roll(half, LANES - 1, 1)
    left = pltpu.roll(half, 1, 1)
    upper = jnp.where(rightmost, jnp.where(tile == 7, 0.0, pltpu.roll(right, 7, 0)), right)
    lower = jnp.where(leftmost, jnp.where(tile == 0, 0.0, pltpu.roll(left, 1, 0)), left)
    return upper - lower


def core_index():
    return lax.rem(lax.axis_index("depth"), 2)


def fetch_kernel(field, outer, sem):
    copy = pltpu.make_async_copy(field.at[pl.ds((field.shape[0] - 1) * core_index(), 1)], outer, sem)
    copy.start()
    copy.wait()


def edge_kernel(own, partner, outer, sent, edge, inner):
    planes, rows, width = partner.shape
    core = core_index()

    def row(plane, tile, n):
        lanes = slice(tile * LANES, (tile + 1) * LANES)

        def mine(slot, at):
            return own[slot, tile, FIRST + at : FIRST + at + 1, :]

        def other(slot, at):
            return partner[slot, at : at + 1, lanes]

        def beyond(slot, at):
            return outer[0, at : at + 1, lanes]

        if plane == 2 * planes:
            at_core0 = at_core1 = beyond
        else:
            at_core0, at_core1 = (mine, other) if plane < planes else (other, mine)
        return jnp.where(core == 0, at_core0(plane % planes, n), at_core1(plane % planes, rows - 1 - n))

    for plane in range(2 * planes + 1):
        for tile in range(width // LANES):
            at = plane * (width // LANES) + tile
            edge[at : at + 1, :] = row(plane, tile, 0)
            inner[at : at + 1, :] = row(plane, tile, 1)
            sent[at : at + 1, :] = row(plane, tile, rows - 1)


def start_state():
    zero = jnp.zeros((8, LANES), jnp.float32)
    return zero, zero + 1.0, zero, zero, zero


def picker(buf, core):
    def picked(plane, tile, group, offset):
        return buf[plane, tile, pl.ds(FIRST + 48 * group + 3 * core + offset, 8, stride=6), :]

    return picked


def plane_differences(picked, plane, tile, tiles, group, rows):
    leftmost, rightmost = lane_masks()
    left, right = jnp.where(tile == 0, tiles, tile - 1), tile + 1
    return [
        pltpu.roll(jnp.where(leftmost, picked(plane, right, group, n), row), LANES - 1, 1)
        - pltpu.roll(jnp.where(rightmost, picked(plane, left, group, n), row), 1, 1)
        for n, row in enumerate(rows)
    ]


def shade_tile(spacing, picked, samples, tile, tiles, group, last=False):
    low = [picked(samples.start, tile, group, offset) for offset in range(-1, 4)]
    low_cols = plane_differences(picked, samples.start, tile, tiles, group, low[1:4])
    states = [start_state()] * 3
    for plane in samples:
        if last:
            high, high_cols = [jnp.zeros_like(low[0])] * 5, [jnp.zeros_like(low[0])] * 3
        else:
            high = [picked(plane + 1, tile, group, offset) for offset in range(-1, 4)]
            high_cols = plane_differences(picked, plane + 1, tile, tiles, group, high[1:4])
        half = [0.25 * (a + b) for a, b in zip(low, high)]
        for row in range(3):
            states[row] = sample_step(
                spacing,
                states[row],
                low[row + 1],
                high[row + 1],
                half[row + 1],
                half[row],
                half[row + 2],
                0.25 * (low_cols[row] + high_cols[row]),
            )
        low, low_cols = high, high_cols
    return states


def join(first, nearer, farther):
    near_through, *near_sums = nearer
    far_through, *far_sums = farther
    on_near = jnp.where(first, 1.0, far_through)
    on_far = jnp.where(first, near_through, 1.0)
    return (near_through * far_through, *[on_near * a + on_far * b for a, b in zip(near_sums, far_sums)])


def own_kernel(spacing, field, own, sums, sems):
    planes, rows, width = field.shape
    tiles = width // LANES
    copies = [
        pltpu.make_async_copy(
            field.at[:, :, pl.ds(tile * LANES, LANES)], own.at[:, tile, pl.ds(FIRST, rows), :], sems.at[tile]
        )
        for tile in range(tiles)
    ]
    for copy in copies:
        copy.start()
    own[:, tiles, :, :] = jnp.zeros((planes, PITCH, LANES), jnp.float32)
    for copy in copies:
        copy.wait()
    picked = picker(own, core_index())

    def step(index, carry):
        group, tile = index // tiles, lax.rem(index, tiles)
        for row, state in enumerate(shade_tile(spacing, picked, range(planes - 1), tile, tiles, group)):
            for n, value in enumerate(state[1:]):
                sums[n, group * 3 + row, pl.ds(tile * 8, 8), :] = value
        return carry

    lax.fori_loop(0, sums.shape[1] // 3 * tiles, step, 0)


def partner_kernel(spacing, group, own, partner, own_sums, sums, buf):
    planes, _, width = partner.shape
    tiles = width // LANES
    core = core_index()
    first = 40 * group
    padded = slice(FIRST + first, FIRST + first + 56)
    for tile in range(tiles):
        for plane in range(planes):
            lanes = slice(tile * LANES, (tile + 1) * LANES)
            buf[plane + 1 - core, tile, padded, :] = partner[plane, first : first + 56, lanes]
        buf[planes * core, tile, :, :] = jnp.where(core == 0, own[planes - 1, tile], own[0, tile])
    buf[:, tiles, :, :] = jnp.zeros((planes + 1, PITCH, LANES), jnp.float32)
    picked = picker(buf, core)

    def step(tile, carry):
        part = pl.ds(tile * 8, 8)
        for row, state in enumerate(shade_tile(spacing, picked, range(planes), tile, tiles, group)):
            nearer = tuple(own_sums[n, group * 3 + row, part, :] for n in range(4))
            for n, value in enumerate(join(core == 0, nearer, state[1:])):
                sums[n, row, part, :] = value
        return carry

    lax.fori_loop(0, tiles, step, 0)

    @pl.when(lax.axis_index("depth") == lax.axis_size("depth") - 2)
    def _():
        def last_step(tile, carry):
            part = pl.ds(tile * 8, 8)
            last = range(planes, planes + 1)
            for row, state in enumerate(shade_tile(spacing, picked, last, tile, tiles, group, last=True)):
                nearer = tuple(sums[n, row, part, :] for n in range(4))
                for n, value in enumerate(join(True, nearer, state[1:])):
                    sums[n, row, part, :] = value
            return carry

        lax.fori_loop(0, tiles, last_step, 0)


def finished(core, present, bulk, outer):
    outer = (jnp.where(present, outer[0], 1.0), *[jnp.where(present, value, 0.0) for value in outer[1:]])
    through, total, tilt, middle = join(core == 1, bulk, outer)
    return 0.5 * (total + tilt), middle, 0.5 * (total - tilt), through


def outer_kernel(spacing, sums0, sums1, own, outer, out, buf):
    slots, tiles = own.shape[0], own.shape[1] - 1
    rows = outer.shape[1]
    core = core_index()
    present = lax.axis_index("depth") != 0
    for tile in range(tiles):
        buf[0, tile, FIRST : FIRST + rows, :] = outer[0, :, tile * LANES : (tile + 1) * LANES]
    buf[:, tiles, :, :] = jnp.zeros((1, PITCH, LANES), jnp.float32)
    to_high = jnp.where(core == 0, -1.0, 1.0)
    near_picked, far_picked = picker(own, core), picker(buf, core)
    nearest = (slots - 1) * core

    def shade(tile, carry):
        part = pl.ds(tile * 8, 8)
        for group, sums in enumerate((sums0, sums1)):
            near = [near_picked(nearest, tile, group, offset) for offset in range(-1, 4)]
            far = [far_picked(0, tile, group, offset) for offset in range(-1, 4)]
            near_cols = plane_differences(near_picked, nearest, tile, tiles, group, near[1:4])
            far_cols = plane_differences(far_picked, 0, tile, tiles, group, far[1:4])
            half = [0.25 * (a + b) for a, b in zip(near, far)]
            for row in range(3):
                sample = sample_step(
                    spacing,
                    start_state(),
                    to_high * near[row + 1],
                    to_high * far[row + 1],
                    half[row + 1],
                    half[row],
                    half[row + 2],
                    0.25 * (near_cols[row] + far_cols[row]),
                )
                bulk = tuple(sums[n, row, part, :] for n in range(4))
                for channel, value in enumerate(finished(core, present, bulk, sample[1:])):
                    out[pl.ds(group * 768 + row * 32 + channel * 8 + tile, 8, stride=96), :] = value
        return carry

    lax.fori_loop(0, tiles, shade, 0)


def line_kernel(spacing, main, edge, inner, beside, out, strip, sem):
    del main
    core = core_index()
    present = lax.axis_index("depth") != 0
    planes = edge.shape[0] // 8 - 1

    def plane_rows(plane):
        at = slice(plane * 8, plane * 8 + 8)
        return edge[at, :], inner[at, :], beside[at, :]

    def line_step(line, low, high):
        half, within, beyond = [0.25 * (a + b) for a, b in zip(low, high)]
        above = jnp.where(core == 0, beyond, within)
        below = jnp.where(core == 0, within, beyond)
        return sample_step(spacing, line, low[0], high[0], half, above, below, row_slopes(half))

    line = start_state()
    for plane in range(planes - 1):
        line = line_step(line, plane_rows(plane), plane_rows(plane + 1))
    zero = jnp.zeros((8, LANES), jnp.float32)
    ended = line_step(line, plane_rows(planes - 1), (zero, zero, zero))
    at_end = lax.axis_index("depth") == lax.axis_size("depth") - 2
    line = tuple(jnp.where(at_end, a, b) for a, b in zip(ended, line))
    far = plane_rows(planes)
    near = [jnp.where(core == 0, a, b) for a, b in zip(plane_rows(0), plane_rows(planes - 1))]
    low = [jnp.where(core == 0, b, a) for a, b in zip(near, far)]
    high = [jnp.where(core == 0, a, b) for a, b in zip(near, far)]
    sample = line_step(start_state(), low, high)
    for channel, value in enumerate(finished(core, present, line[1:], sample[1:])):
        strip[channel * 8 : channel * 8 + 8, :] = value
    place = pl.multiple_of(core * (out.shape[0] - 32), 8)
    copy = pltpu.make_async_copy(strip, out.at[pl.ds(place, 32)], sem)
    copy.start()
    copy.wait()


def blend_kernel(slabs, out):
    count = slabs.shape[0] // 96
    for row in range(3):
        through = jnp.ones((8, LANES), jnp.float32)
        colour = [jnp.zeros((8, LANES), jnp.float32)] * 3
        for slab in range(count):
            base = slab * 96 + row * 32
            for channel in range(3):
                colour[channel] = colour[channel] + through * slabs[base + channel * 8 : base + channel * 8 + 8, :]
            through = through * slabs[base + 24 : base + 32, :]
        for channel, value in enumerate((*colour, 1.0 - through)):
            for tile in range(8):
                out[row, channel : channel + 1, tile * LANES : (tile + 1) * LANES] = value[tile : tile + 1, :]


def f32(*shape):
    return jax.ShapeDtypeStruct(shape, jnp.float32)


def cost(flops, size):
    return pl.CostEstimate(flops=flops, bytes_accessed=size, transcendentals=0)


def composited(field):
    planes, rows, width = field.shape
    depth = lax.axis_size("depth")
    strips = lax.axis_size("tile")
    chips = depth // 2
    tiles = width // LANES
    spacing = 3.0 / (planes * depth)

    outer_out = pl.pallas_call(
        fetch_kernel,
        out_shape=f32(1, rows, width),
        in_specs=[pl.BlockSpec(memory_space=pltpu.HBM)],
        out_specs=VMEM,
        scratch_shapes=[pltpu.SemaphoreType.DMA],
        compiler_params=pltpu.CompilerParams(vmem_limit_bytes=4 << 20),
        cost_estimate=cost(1 << 10, 1 << 20),
        name="fetch",
    )(field)
    outer = lax.ppermute(
        outer_out,
        "depth",
        [(2 * k + 1, 2 * k + 2) for k in range(chips - 1)] + [(2 * k + 2, 2 * k + 1) for k in range(chips - 1)],
    )
    partner = lax.ppermute(field, "depth", [(i, i ^ 1) for i in range(depth)])

    own, own_sums = pl.pallas_call(
        functools.partial(own_kernel, spacing),
        out_shape=(f32(planes, tiles + 1, PITCH, LANES), f32(4, rows // 16, tiles * 8, LANES)),
        in_specs=[pl.BlockSpec(memory_space=pltpu.HBM)],
        out_specs=(VMEM, VMEM),
        scratch_shapes=[pltpu.SemaphoreType.DMA((tiles,))],
        compiler_params=pltpu.CompilerParams(vmem_limit_bytes=12 << 20),
        cost_estimate=cost(1 << 26, 1 << 21),
        name="own",
    )(field)

    lines = (2 * planes + 1) * tiles
    sent, edge, inner = pl.pallas_call(
        edge_kernel,
        out_shape=(f32(lines, LANES), f32(lines, LANES), f32(lines, LANES)),
        in_specs=[VMEM, VMEM, VMEM],
        out_specs=(VMEM, VMEM, VMEM),
        compiler_params=pltpu.CompilerParams(vmem_limit_bytes=4 << 20),
        cost_estimate=cost(1 << 20, 1 << 19),
        name="edges",
    )(own, partner, outer)
    place = lambda d, s: d * strips + s
    beside = lax.ppermute(
        sent,
        ("depth", "tile"),
        [(place(2 * k, t), place(2 * k, t + 1)) for k in range(chips) for t in range(strips - 1)]
        + [(place(2 * k + 1, t + 1), place(2 * k + 1, t)) for k in range(chips) for t in range(strips - 1)],
    )

    sums = []
    for group in range(2):
        sums.append(
            pl.pallas_call(
                functools.partial(partner_kernel, spacing, group),
                out_shape=f32(4, 3, tiles * 8, LANES),
                in_specs=[VMEM] * 3,
                out_specs=VMEM,
                scratch_shapes=[pltpu.VMEM((planes + 1, tiles + 1, PITCH, LANES), jnp.float32)],
                compiler_params=pltpu.CompilerParams(vmem_limit_bytes=12 << 20),
                cost_estimate=cost(1 << 25, 1 << 20),
            )(own, partner, own_sums)
        )
    most = pl.pallas_call(
        functools.partial(outer_kernel, spacing),
        out_shape=f32(chips * 96, LANES),
        in_specs=[VMEM] * 4,
        out_specs=VMEM,
        scratch_shapes=[pltpu.VMEM((1, tiles + 1, PITCH, LANES), jnp.float32)],
        compiler_params=pltpu.CompilerParams(vmem_limit_bytes=12 << 20),
        cost_estimate=cost(1 << 24, 1 << 21),
        name="outer",
    )(*sums, own, outer)
    parts = pl.pallas_call(
        functools.partial(line_kernel, spacing),
        out_shape=f32(chips * 96, LANES),
        in_specs=[pl.BlockSpec(memory_space=pl.ANY)] + [VMEM] * 3,
        out_specs=pl.BlockSpec(memory_space=pl.ANY),
        input_output_aliases={0: 0},
        scratch_shapes=[pltpu.VMEM((32, LANES), jnp.float32), pltpu.SemaphoreType.DMA],
        compiler_params=pltpu.CompilerParams(vmem_limit_bytes=4 << 20),
        cost_estimate=cost(1 << 20, 1 << 18),
        name="line",
    )(most, edge, inner, beside)
    slabs = lax.all_to_all(
        parts.reshape(chips, 96, LANES),
        "depth",
        split_axis=0,
        concat_axis=0,
        tiled=True,
        axis_index_groups=[[2 * k + c for k in range(chips)] for c in range(2)],
    )
    image = pl.pallas_call(
        blend_kernel,
        out_shape=f32(3, 4, width),
        in_specs=[VMEM],
        out_specs=VMEM,
        compiler_params=pltpu.CompilerParams(vmem_limit_bytes=8 << 20),
        name="blend",
    )(slabs.reshape(chips * 96, LANES))
    return jnp.transpose(image, (1, 0, 2))


def solution(mesh):
    return jax.shard_map(
        composited,
        mesh=mesh,
        in_specs=(P("depth", "tile", None),),
        out_specs=P(None, ("tile", "depth"), None),
        check_vma=False,
    )
```

```python
import functools
import math

import jax
import jax.numpy as jnp
from jax import lax
from jax.experimental import pallas as pl
from jax.experimental.pallas import tpu as pltpu
from jax.sharding import PartitionSpec as P


centres = (-1.2, 0.3, 1.5)
spreads = (0.25, 0.35, 0.3)
heights = (2.0, 1.0, 3.0)
floor_density = 0.05
light_cols = 0.48
light_rows = 0.6
light_depth = 0.64

LANES = 128
LOG2E = math.log2(math.e)
SHINE = 0.7 * light_cols
FIRST = 8
PITCH = 112
VMEM = pl.BlockSpec(memory_space=pltpu.VMEM)


def sample_step(spacing, state, low, high, twice, above, below, columns):
    run, through, total, tilt, middle = state
    run = run - spacing * LOG2E * floor_density
    for centre, spread, bump in zip(centres, spreads, heights):
        offset = twice - 2.0 * centre
        run = run - jnp.exp2(
            (offset * offset) * (-0.25 * LOG2E / (spread * spread)) + math.log2(bump * spacing * LOG2E)
        )
    now = jnp.exp2(run)
    weight = through - now
    rise = below - above
    depth = high - low
    facing = columns + (light_rows / light_cols) * rise + (4.0 * light_depth / light_cols) * depth
    length = columns * columns + rise * rise + (16.0 * (depth * depth) + 16.0)
    lit = weight * (0.3 / SHINE + jnp.abs(facing) * lax.rsqrt(length))
    total = total + lit
    tilt = tilt + lit * jnp.tanh(0.5 * twice)
    middle = middle + lit * jnp.exp2((twice * twice) * (-0.25 * LOG2E))
    return run, now, total, tilt, middle


def lane_masks():
    lane = lax.broadcasted_iota(jnp.int32, (8, LANES), 1)
    return lane == 0, lane == LANES - 1


def row_slopes(half):
    leftmost, rightmost = lane_masks()
    tile = lax.broadcasted_iota(jnp.int32, (8, LANES), 0)
    right = pltpu.roll(half, LANES - 1, 1)
    left = pltpu.roll(half, 1, 1)
    upper = jnp.where(rightmost, jnp.where(tile == 7, 0.0, pltpu.roll(right, 7, 0)), right)
    lower = jnp.where(leftmost, jnp.where(tile == 0, 0.0, pltpu.roll(left, 1, 0)), left)
    return upper - lower


def core_index():
    return lax.rem(lax.axis_index("depth"), 2)


def fetch_kernel(field, outer, sem):
    copy = pltpu.make_async_copy(field.at[pl.ds((field.shape[0] - 1) * core_index(), 1)], outer, sem)
    copy.start()
    copy.wait()


def edge_kernel(own, partner, outer, sent, edge, inner):
    planes, rows, width = partner.shape
    core = core_index()

    def row(plane, tile, n):
        lanes = slice(tile * LANES, (tile + 1) * LANES)

        def mine(slot, at):
            return own[slot, tile, FIRST + at : FIRST + at + 1, :]

        def other(slot, at):
            return partner[slot, at : at + 1, lanes]

        def beyond(slot, at):
            return outer[0, at : at + 1, lanes]

        if plane == 2 * planes:
            at_core0 = at_core1 = beyond
        else:
            at_core0, at_core1 = (mine, other) if plane < planes else (other, mine)
        return jnp.where(core == 0, at_core0(plane % planes, n), at_core1(plane % planes, rows - 1 - n))

    for plane in range(2 * planes + 1):
        for tile in range(width // LANES):
            at = plane * (width // LANES) + tile
            edge[at : at + 1, :] = row(plane, tile, 0)
            inner[at : at + 1, :] = row(plane, tile, 1)
            sent[at : at + 1, :] = row(plane, tile, rows - 1)


def start_state():
    zero = jnp.zeros((8, LANES), jnp.float32)
    return zero, zero + 1.0, zero, zero, zero


def picker(buf, core):
    def picked(plane, tile, group, offset):
        return buf[plane, tile, pl.ds(FIRST + 48 * group + 3 * core + offset, 8, stride=6), :]

    return picked


def plane_differences(picked, plane, tile, tiles, group, rows):
    leftmost, rightmost = lane_masks()
    left, right = jnp.where(tile == 0, tiles, tile - 1), tile + 1
    return [
        pltpu.roll(jnp.where(leftmost, picked(plane, right, group, n), row), LANES - 1, 1)
        - pltpu.roll(jnp.where(rightmost, picked(plane, left, group, n), row), 1, 1)
        for n, row in enumerate(rows)
    ]


def shade_tile(spacing, picked, samples, tile, tiles, group, last=False):
    low = [picked(samples.start, tile, group, offset) for offset in range(-1, 4)]
    low_cols = plane_differences(picked, samples.start, tile, tiles, group, low[1:4])
    states = [start_state()] * 3
    for plane in samples:
        if last:
            high, high_cols = [jnp.zeros_like(low[0])] * 5, [jnp.zeros_like(low[0])] * 3
        else:
            high = [picked(plane + 1, tile, group, offset) for offset in range(-1, 4)]
            high_cols = plane_differences(picked, plane + 1, tile, tiles, group, high[1:4])
        twice = [a + b for a, b in zip(low, high)]
        for row in range(3):
            states[row] = sample_step(
                spacing,
                states[row],
                low[row + 1],
                high[row + 1],
                twice[row + 1],
                twice[row],
                twice[row + 2],
                low_cols[row] + high_cols[row],
            )
        low, low_cols = high, high_cols
    return states


def join(first, nearer, farther):
    near_through, *near_sums = nearer
    far_through, *far_sums = farther
    on_near = jnp.where(first, 1.0, far_through)
    on_far = jnp.where(first, near_through, 1.0)
    return (near_through * far_through, *[on_near * a + on_far * b for a, b in zip(near_sums, far_sums)])


def own_kernel(spacing, field, own, sums, sems):
    planes, rows, width = field.shape
    tiles = width // LANES
    copies = [
        pltpu.make_async_copy(
            field.at[:, :, pl.ds(tile * LANES, LANES)], own.at[:, tile, pl.ds(FIRST, rows), :], sems.at[tile]
        )
        for tile in range(tiles)
    ]
    for copy in copies:
        copy.start()
    own[:, tiles, :, :] = jnp.zeros((planes, PITCH, LANES), jnp.float32)
    for copy in copies:
        copy.wait()
    picked = picker(own, core_index())

    def step(tile, carry):
        part = pl.ds(tile * 8, 8)
        for group in range(sums.shape[1] // 3):
            for row, state in enumerate(shade_tile(spacing, picked, range(planes - 1), tile, tiles, group)):
                for n, value in enumerate(state[1:]):
                    sums[n, group * 3 + row, part, :] = value
        return carry

    lax.fori_loop(0, tiles, step, 0)


def partner_kernel(spacing, group, own, partner, own_sums, sums, buf):
    planes, _, width = partner.shape
    tiles = width // LANES
    core = core_index()
    first = 40 * group
    padded = slice(FIRST + first, FIRST + first + 56)
    for tile in range(tiles):
        for plane in range(planes):
            lanes = slice(tile * LANES, (tile + 1) * LANES)
            buf[plane + 1 - core, tile, padded, :] = partner[plane, first : first + 56, lanes]
        buf[planes * core, tile, :, :] = jnp.where(core == 0, own[planes - 1, tile], own[0, tile])
    buf[:, tiles, :, :] = jnp.zeros((planes + 1, PITCH, LANES), jnp.float32)
    picked = picker(buf, core)

    def step(pair, carry):
        for tile in (2 * pair, 2 * pair + 1):
            part = pl.ds(tile * 8, 8)
            for row, state in enumerate(shade_tile(spacing, picked, range(planes), tile, tiles, group)):
                nearer = tuple(own_sums[n, group * 3 + row, part, :] for n in range(4))
                for n, value in enumerate(join(core == 0, nearer, state[1:])):
                    sums[n, row, part, :] = value
        return carry

    lax.fori_loop(0, tiles // 2, step, 0)

    @pl.when(lax.axis_index("depth") == lax.axis_size("depth") - 2)
    def _():
        def last_step(tile, carry):
            part = pl.ds(tile * 8, 8)
            last = range(planes, planes + 1)
            for row, state in enumerate(shade_tile(spacing, picked, last, tile, tiles, group, last=True)):
                nearer = tuple(sums[n, row, part, :] for n in range(4))
                for n, value in enumerate(join(True, nearer, state[1:])):
                    sums[n, row, part, :] = value
            return carry

        lax.fori_loop(0, tiles, last_step, 0)


def finished(core, present, bulk, outer):
    outer = (jnp.where(present, outer[0], 1.0), *[jnp.where(present, value, 0.0) for value in outer[1:]])
    through, total, tilt, middle = join(core == 1, bulk, outer)
    return (0.5 * SHINE) * (total + tilt), SHINE * middle, (0.5 * SHINE) * (total - tilt), through


def outer_kernel(spacing, sums0, sums1, own, outer, out, buf):
    slots, tiles = own.shape[0], own.shape[1] - 1
    rows = outer.shape[1]
    core = core_index()
    present = lax.axis_index("depth") != 0
    for tile in range(tiles):
        buf[0, tile, FIRST : FIRST + rows, :] = outer[0, :, tile * LANES : (tile + 1) * LANES]
    buf[:, tiles, :, :] = jnp.zeros((1, PITCH, LANES), jnp.float32)
    to_high = jnp.where(core == 0, -1.0, 1.0)
    near_picked, far_picked = picker(own, core), picker(buf, core)
    nearest = (slots - 1) * core

    def shade(tile, carry):
        part = pl.ds(tile * 8, 8)
        for group, sums in enumerate((sums0, sums1)):
            near = [near_picked(nearest, tile, group, offset) for offset in range(-1, 4)]
            far = [far_picked(0, tile, group, offset) for offset in range(-1, 4)]
            near_cols = plane_differences(near_picked, nearest, tile, tiles, group, near[1:4])
            far_cols = plane_differences(far_picked, 0, tile, tiles, group, far[1:4])
            twice = [a + b for a, b in zip(near, far)]
            for row in range(3):
                sample = sample_step(
                    spacing,
                    start_state(),
                    to_high * near[row + 1],
                    to_high * far[row + 1],
                    twice[row + 1],
                    twice[row],
                    twice[row + 2],
                    near_cols[row] + far_cols[row],
                )
                bulk = tuple(sums[n, row, part, :] for n in range(4))
                for channel, value in enumerate(finished(core, present, bulk, sample[1:])):
                    out[pl.ds(group * 768 + row * 32 + channel * 8 + tile, 8, stride=96), :] = value
        return carry

    lax.fori_loop(0, tiles, shade, 0)


def line_kernel(spacing, main, edge, inner, beside, out, strip, sem):
    del main
    core = core_index()
    present = lax.axis_index("depth") != 0
    planes = edge.shape[0] // 8 - 1

    def plane_rows(plane):
        at = slice(plane * 8, plane * 8 + 8)
        return edge[at, :], inner[at, :], beside[at, :]

    def line_step(line, low, high):
        twice, within, beyond = [a + b for a, b in zip(low, high)]
        above = jnp.where(core == 0, beyond, within)
        below = jnp.where(core == 0, within, beyond)
        return sample_step(spacing, line, low[0], high[0], twice, above, below, row_slopes(twice))

    line = start_state()
    for plane in range(planes - 1):
        line = line_step(line, plane_rows(plane), plane_rows(plane + 1))
    zero = jnp.zeros((8, LANES), jnp.float32)
    ended = line_step(line, plane_rows(planes - 1), (zero, zero, zero))
    at_end = lax.axis_index("depth") == lax.axis_size("depth") - 2
    line = tuple(jnp.where(at_end, a, b) for a, b in zip(ended, line))
    far = plane_rows(planes)
    near = [jnp.where(core == 0, a, b) for a, b in zip(plane_rows(0), plane_rows(planes - 1))]
    low = [jnp.where(core == 0, b, a) for a, b in zip(near, far)]
    high = [jnp.where(core == 0, a, b) for a, b in zip(near, far)]
    sample = line_step(start_state(), low, high)
    for channel, value in enumerate(finished(core, present, line[1:], sample[1:])):
        strip[channel * 8 : channel * 8 + 8, :] = value
    place = pl.multiple_of(core * (out.shape[0] - 32), 8)
    copy = pltpu.make_async_copy(strip, out.at[pl.ds(place, 32)], sem)
    copy.start()
    copy.wait()


def blend_kernel(slabs, out):
    count = slabs.shape[0] // 96
    for row in range(3):
        through = jnp.ones((8, LANES), jnp.float32)
        colour = [jnp.zeros((8, LANES), jnp.float32)] * 3
        for slab in range(count):
            base = slab * 96 + row * 32
            for channel in range(3):
                colour[channel] = colour[channel] + through * slabs[base + channel * 8 : base + channel * 8 + 8, :]
            through = through * slabs[base + 24 : base + 32, :]
        for channel, value in enumerate((*colour, 1.0 - through)):
            for tile in range(8):
                out[row, channel : channel + 1, tile * LANES : (tile + 1) * LANES] = value[tile : tile + 1, :]


def f32(*shape):
    return jax.ShapeDtypeStruct(shape, jnp.float32)


def cost(flops, size):
    return pl.CostEstimate(flops=flops, bytes_accessed=size, transcendentals=0)


def composited(field):
    planes, rows, width = field.shape
    depth = lax.axis_size("depth")
    strips = lax.axis_size("tile")
    chips = depth // 2
    tiles = width // LANES
    spacing = 3.0 / (planes * depth)

    outer_out = pl.pallas_call(
        fetch_kernel,
        out_shape=f32(1, rows, width),
        in_specs=[pl.BlockSpec(memory_space=pltpu.HBM)],
        out_specs=VMEM,
        scratch_shapes=[pltpu.SemaphoreType.DMA],
        compiler_params=pltpu.CompilerParams(vmem_limit_bytes=4 << 20),
        cost_estimate=cost(1 << 10, 1 << 20),
        name="fetch",
    )(field)
    outer = lax.ppermute(
        outer_out,
        "depth",
        [(2 * k + 1, 2 * k + 2) for k in range(chips - 1)] + [(2 * k + 2, 2 * k + 1) for k in range(chips - 1)],
    )
    partner = lax.ppermute(field, "depth", [(i, i ^ 1) for i in range(depth)])

    own, own_sums = pl.pallas_call(
        functools.partial(own_kernel, spacing),
        out_shape=(f32(planes, tiles + 1, PITCH, LANES), f32(4, rows // 16, tiles * 8, LANES)),
        in_specs=[pl.BlockSpec(memory_space=pltpu.HBM)],
        out_specs=(VMEM, VMEM),
        scratch_shapes=[pltpu.SemaphoreType.DMA((tiles,))],
        compiler_params=pltpu.CompilerParams(vmem_limit_bytes=12 << 20),
        cost_estimate=cost(1 << 26, 1 << 21),
        name="own",
    )(field)

    lines = (2 * planes + 1) * tiles
    sent, edge, inner = pl.pallas_call(
        edge_kernel,
        out_shape=(f32(lines, LANES), f32(lines, LANES), f32(lines, LANES)),
        in_specs=[VMEM, VMEM, VMEM],
        out_specs=(VMEM, VMEM, VMEM),
        compiler_params=pltpu.CompilerParams(vmem_limit_bytes=4 << 20),
        cost_estimate=cost(1 << 20, 1 << 19),
        name="edges",
    )(own, partner, outer)
    place = lambda d, s: d * strips + s
    beside = lax.ppermute(
        sent,
        ("depth", "tile"),
        [(place(2 * k, t), place(2 * k, t + 1)) for k in range(chips) for t in range(strips - 1)]
        + [(place(2 * k + 1, t + 1), place(2 * k + 1, t)) for k in range(chips) for t in range(strips - 1)],
    )

    sums = []
    for group in range(2):
        sums.append(
            pl.pallas_call(
                functools.partial(partner_kernel, spacing, group),
                out_shape=f32(4, 3, tiles * 8, LANES),
                in_specs=[VMEM] * 3,
                out_specs=VMEM,
                scratch_shapes=[pltpu.VMEM((planes + 1, tiles + 1, PITCH, LANES), jnp.float32)],
                compiler_params=pltpu.CompilerParams(vmem_limit_bytes=12 << 20),
                cost_estimate=cost(1 << 25, 1 << 20),
            )(own, partner, own_sums)
        )
    most = pl.pallas_call(
        functools.partial(outer_kernel, spacing),
        out_shape=f32(chips * 96, LANES),
        in_specs=[VMEM] * 4,
        out_specs=VMEM,
        scratch_shapes=[pltpu.VMEM((1, tiles + 1, PITCH, LANES), jnp.float32)],
        compiler_params=pltpu.CompilerParams(vmem_limit_bytes=12 << 20),
        cost_estimate=cost(1 << 24, 1 << 21),
        name="outer",
    )(*sums, own, outer)
    parts = pl.pallas_call(
        functools.partial(line_kernel, spacing),
        out_shape=f32(chips * 96, LANES),
        in_specs=[pl.BlockSpec(memory_space=pl.ANY)] + [VMEM] * 3,
        out_specs=pl.BlockSpec(memory_space=pl.ANY),
        input_output_aliases={0: 0},
        scratch_shapes=[pltpu.VMEM((32, LANES), jnp.float32), pltpu.SemaphoreType.DMA],
        compiler_params=pltpu.CompilerParams(vmem_limit_bytes=4 << 20),
        cost_estimate=cost(1 << 20, 1 << 18),
        name="line",
    )(most, edge, inner, beside)
    slabs = lax.all_to_all(
        parts.reshape(chips, 96, LANES),
        "depth",
        split_axis=0,
        concat_axis=0,
        tiled=True,
        axis_index_groups=[[2 * k + c for k in range(chips)] for c in range(2)],
    )
    image = pl.pallas_call(
        blend_kernel,
        out_shape=f32(3, 4, width),
        in_specs=[VMEM],
        out_specs=VMEM,
        compiler_params=pltpu.CompilerParams(vmem_limit_bytes=8 << 20),
        name="blend",
    )(slabs.reshape(chips * 96, LANES))
    return jnp.transpose(image, (1, 0, 2))


def solution(mesh):
    return jax.shard_map(
        composited,
        mesh=mesh,
        in_specs=(P("depth", "tile", None),),
        out_specs=P(None, ("tile", "depth"), None),
        check_vma=False,
    )
```

```python
import functools
import math

import jax
import jax.numpy as jnp
from jax import lax
from jax.experimental import pallas as pl
from jax.experimental.pallas import tpu as pltpu
from jax.sharding import PartitionSpec as P


centres = (-1.2, 0.3, 1.5)
spreads = (0.25, 0.35, 0.3)
heights = (2.0, 1.0, 3.0)
floor_density = 0.05
light_cols = 0.48
light_rows = 0.6
light_depth = 0.64

LANES = 128
LOG2E = math.log2(math.e)
SHINE = 0.7 * light_cols
FIRST = 8
PITCH = 112
OUTER_ROWS = 80
VMEM = pl.BlockSpec(memory_space=pltpu.VMEM)


def sample_step(spacing, state, low, high, twice, above, below, columns):
    run, through, total, tilt, middle = state
    run = run - spacing * LOG2E * floor_density
    for centre, spread, bump in zip(centres, spreads, heights):
        offset = twice - 2.0 * centre
        run = run - jnp.exp2(
            (offset * offset) * (-0.25 * LOG2E / (spread * spread)) + math.log2(bump * spacing * LOG2E)
        )
    now = jnp.exp2(run)
    weight = through - now
    rise = below - above
    depth = high - low
    facing = columns + (light_rows / light_cols) * rise + (4.0 * light_depth / light_cols) * depth
    length = columns * columns + rise * rise + (16.0 * (depth * depth) + 16.0)
    lit = weight * (0.3 / SHINE + jnp.abs(facing) * lax.rsqrt(length))
    total = total + lit
    tilt = tilt + lit * jnp.tanh(0.5 * twice)
    middle = middle + lit * jnp.exp2((twice * twice) * (-0.25 * LOG2E))
    return run, now, total, tilt, middle


def lane_masks():
    lane = lax.broadcasted_iota(jnp.int32, (8, LANES), 1)
    return lane == 0, lane == LANES - 1


def row_slopes(half):
    leftmost, rightmost = lane_masks()
    tile = lax.broadcasted_iota(jnp.int32, (8, LANES), 0)
    right = pltpu.roll(half, LANES - 1, 1)
    left = pltpu.roll(half, 1, 1)
    upper = jnp.where(rightmost, jnp.where(tile == 7, 0.0, pltpu.roll(right, 7, 0)), right)
    lower = jnp.where(leftmost, jnp.where(tile == 0, 0.0, pltpu.roll(left, 1, 0)), left)
    return upper - lower


def core_index():
    return lax.rem(lax.axis_index("depth"), 2)


def fetch_kernel(field, outer, plane, sems):
    planes, rows, width = field.shape
    core = core_index()
    copies = [
        pltpu.make_async_copy(
            field.at[(planes - 1) * core, :, pl.ds(tile * LANES, LANES)],
            plane.at[0, tile, pl.ds(FIRST, rows), :],
            sems.at[tile],
        )
        for tile in range(width // LANES)
    ]
    for copy in copies:
        copy.start()
    for copy in copies:
        copy.wait()
    picked = picker(plane, 1 - core)
    for tile in range(width // LANES):
        for offset in range(-1, 4):
            for group in range(2):
                outer[outer_row(tile, group, offset), :] = picked(0, tile, group, offset)
        at = OUTER_ROWS * (width // LANES) + tile
        outer[at : at + 1, :] = jnp.where(
            core == 1, plane[0, tile, FIRST + rows - 1 : FIRST + rows, :], plane[0, tile, FIRST : FIRST + 1, :]
        )


def outer_row(tile, group, offset):
    return pl.ds(pl.multiple_of(tile * OUTER_ROWS, 8) + (offset + 1) * 16 + group * 8, 8)


def edge_kernel(own, partner, outer, sent, edge, inner):
    planes, rows, width = partner.shape
    core = core_index()

    def row(plane, tile, n):
        lanes = slice(tile * LANES, (tile + 1) * LANES)

        def mine(slot, at):
            return own[slot, tile, FIRST + at : FIRST + at + 1, :]

        def other(slot, at):
            return partner[slot, at : at + 1, lanes]

        def beyond(slot, at):
            if n == rows - 1:
                at = OUTER_ROWS * (width // LANES) + tile
            else:
                at = tile * OUTER_ROWS + (16 * (at + 1) if at < 8 else 16 * (at + 1 - (rows - 3)) + 15)
            return outer[at : at + 1, :]

        if plane == 2 * planes:
            at_core0 = at_core1 = beyond
        else:
            at_core0, at_core1 = (mine, other) if plane < planes else (other, mine)
        return jnp.where(core == 0, at_core0(plane % planes, n), at_core1(plane % planes, rows - 1 - n))

    for plane in range(2 * planes + 1):
        for tile in range(width // LANES):
            at = plane * (width // LANES) + tile
            edge[at : at + 1, :] = row(plane, tile, 0)
            inner[at : at + 1, :] = row(plane, tile, 1)
            sent[at : at + 1, :] = row(plane, tile, rows - 1)


def start_state():
    zero = jnp.zeros((8, LANES), jnp.float32)
    return zero, zero + 1.0, zero, zero, zero


def picker(buf, core):
    def picked(plane, tile, group, offset):
        return buf[plane, tile, pl.ds(FIRST + 48 * group + 3 * core + offset, 8, stride=6), :]

    return picked


def plane_differences(picked, plane, tile, tiles, group, rows):
    leftmost, rightmost = lane_masks()
    left, right = jnp.where(tile == 0, tiles, tile - 1), tile + 1
    return [
        pltpu.roll(jnp.where(leftmost, picked(plane, right, group, n), row), LANES - 1, 1)
        - pltpu.roll(jnp.where(rightmost, picked(plane, left, group, n), row), 1, 1)
        for n, row in enumerate(rows)
    ]


def shade_tile(spacing, picked, samples, tile, tiles, group, last=False):
    low = [picked(samples.start, tile, group, offset) for offset in range(-1, 4)]
    low_cols = plane_differences(picked, samples.start, tile, tiles, group, low[1:4])
    states = [start_state()] * 3
    for plane in samples:
        if last:
            high, high_cols = [jnp.zeros_like(low[0])] * 5, [jnp.zeros_like(low[0])] * 3
        else:
            high = [picked(plane + 1, tile, group, offset) for offset in range(-1, 4)]
            high_cols = plane_differences(picked, plane + 1, tile, tiles, group, high[1:4])
        twice = [a + b for a, b in zip(low, high)]
        for row in range(3):
            states[row] = sample_step(
                spacing,
                states[row],
                low[row + 1],
                high[row + 1],
                twice[row + 1],
                twice[row],
                twice[row + 2],
                low_cols[row] + high_cols[row],
            )
        low, low_cols = high, high_cols
    return states


def join(first, nearer, farther):
    near_through, *near_sums = nearer
    far_through, *far_sums = farther
    on_near = jnp.where(first, 1.0, far_through)
    on_far = jnp.where(first, near_through, 1.0)
    return (near_through * far_through, *[on_near * a + on_far * b for a, b in zip(near_sums, far_sums)])


def own_kernel(spacing, field, own, sums, sems):
    planes, rows, width = field.shape
    tiles = width // LANES
    copies = [
        pltpu.make_async_copy(
            field.at[:, :, pl.ds(tile * LANES, LANES)], own.at[:, tile, pl.ds(FIRST, rows), :], sems.at[tile]
        )
        for tile in range(tiles)
    ]
    for copy in copies:
        copy.start()
    own[:, tiles, :, :] = jnp.zeros((planes, PITCH, LANES), jnp.float32)
    for copy in copies:
        copy.wait()
    picked = picker(own, core_index())

    def step(tile, carry):
        part = pl.ds(tile * 8, 8)
        for group in range(sums.shape[1] // 3):
            for row, state in enumerate(shade_tile(spacing, picked, range(planes - 1), tile, tiles, group)):
                for n, value in enumerate(state[1:]):
                    sums[n, group * 3 + row, part, :] = value
        return carry

    lax.fori_loop(0, tiles, step, 0)


def partner_kernel(spacing, group, own, partner, own_sums, sums, buf):
    planes, _, width = partner.shape
    tiles = width // LANES
    core = core_index()
    first = 40 * group
    padded = slice(FIRST + first, FIRST + first + 56)
    for tile in range(tiles):
        for plane in range(planes):
            lanes = slice(tile * LANES, (tile + 1) * LANES)
            buf[plane + 1 - core, tile, padded, :] = partner[plane, first : first + 56, lanes]
        buf[planes * core, tile, :, :] = jnp.where(core == 0, own[planes - 1, tile], own[0, tile])
    buf[:, tiles, :, :] = jnp.zeros((planes + 1, PITCH, LANES), jnp.float32)
    picked = picker(buf, core)

    def step(pair, carry):
        for tile in (2 * pair, 2 * pair + 1):
            part = pl.ds(tile * 8, 8)
            for row, state in enumerate(shade_tile(spacing, picked, range(planes), tile, tiles, group)):
                nearer = tuple(own_sums[n, group * 3 + row, part, :] for n in range(4))
                for n, value in enumerate(join(core == 0, nearer, state[1:])):
                    sums[n, row, part, :] = value
        return carry

    lax.fori_loop(0, tiles // 2, step, 0)

    @pl.when(lax.axis_index("depth") == lax.axis_size("depth") - 2)
    def _():
        def last_step(turn, carry):
            for tile in [4 * turn + n for n in range(4)]:
                part = pl.ds(tile * 8, 8)
                last = range(planes, planes + 1)
                for row, state in enumerate(shade_tile(spacing, picked, last, tile, tiles, group, last=True)):
                    nearer = tuple(sums[n, row, part, :] for n in range(4))
                    for n, value in enumerate(join(True, nearer, state[1:])):
                        sums[n, row, part, :] = value
            return carry

        lax.fori_loop(0, tiles // 4, last_step, 0)


def finished(core, present, bulk, outer):
    outer = (jnp.where(present, outer[0], 1.0), *[jnp.where(present, value, 0.0) for value in outer[1:]])
    through, total, tilt, middle = join(core == 1, bulk, outer)
    return (0.5 * SHINE) * (total + tilt), SHINE * middle, (0.5 * SHINE) * (total - tilt), through


def outer_kernel(spacing, sums0, sums1, own, outer, out, buf):
    slots, tiles = own.shape[0], own.shape[1] - 1
    core = core_index()
    present = lax.axis_index("depth") != 0
    buf[0 : tiles * OUTER_ROWS, :] = outer[0 : tiles * OUTER_ROWS, :]
    buf[tiles * OUTER_ROWS :, :] = jnp.zeros((OUTER_ROWS, LANES), jnp.float32)
    to_high = jnp.where(core == 0, -1.0, 1.0)
    near_picked = picker(own, core)

    def far_picked(plane, tile, group, offset):
        return buf[outer_row(tile, group, offset), :]

    nearest = (slots - 1) * core

    def shade(tile, carry):
        part = pl.ds(tile * 8, 8)
        for group, sums in enumerate((sums0, sums1)):
            near = [near_picked(nearest, tile, group, offset) for offset in range(-1, 4)]
            far = [far_picked(0, tile, group, offset) for offset in range(-1, 4)]
            near_cols = plane_differences(near_picked, nearest, tile, tiles, group, near[1:4])
            far_cols = plane_differences(far_picked, 0, tile, tiles, group, far[1:4])
            twice = [a + b for a, b in zip(near, far)]
            for row in range(3):
                sample = sample_step(
                    spacing,
                    start_state(),
                    to_high * near[row + 1],
                    to_high * far[row + 1],
                    twice[row + 1],
                    twice[row],
                    twice[row + 2],
                    near_cols[row] + far_cols[row],
                )
                bulk = tuple(sums[n, row, part, :] for n in range(4))
                for channel, value in enumerate(finished(core, present, bulk, sample[1:])):
                    out[pl.ds(group * 768 + row * 32 + channel * 8 + tile, 8, stride=96), :] = value
        return carry

    lax.fori_loop(0, tiles, shade, 0)


def line_kernel(spacing, main, edge, inner, beside, out, strip, sem):
    del main
    core = core_index()
    present = lax.axis_index("depth") != 0
    planes = edge.shape[0] // 8 - 1

    def plane_rows(plane):
        at = slice(plane * 8, plane * 8 + 8)
        return edge[at, :], inner[at, :], beside[at, :]

    def line_step(line, low, high):
        twice, within, beyond = [a + b for a, b in zip(low, high)]
        above = jnp.where(core == 0, beyond, within)
        below = jnp.where(core == 0, within, beyond)
        return sample_step(spacing, line, low[0], high[0], twice, above, below, row_slopes(twice))

    line = start_state()
    for plane in range(planes - 1):
        line = line_step(line, plane_rows(plane), plane_rows(plane + 1))
    zero = jnp.zeros((8, LANES), jnp.float32)
    ended = line_step(line, plane_rows(planes - 1), (zero, zero, zero))
    at_end = lax.axis_index("depth") == lax.axis_size("depth") - 2
    line = tuple(jnp.where(at_end, a, b) for a, b in zip(ended, line))
    far = plane_rows(planes)
    near = [jnp.where(core == 0, a, b) for a, b in zip(plane_rows(0), plane_rows(planes - 1))]
    low = [jnp.where(core == 0, b, a) for a, b in zip(near, far)]
    high = [jnp.where(core == 0, a, b) for a, b in zip(near, far)]
    sample = line_step(start_state(), low, high)
    for channel, value in enumerate(finished(core, present, line[1:], sample[1:])):
        strip[channel * 8 : channel * 8 + 8, :] = value
    place = pl.multiple_of(core * (out.shape[0] - 32), 8)
    copy = pltpu.make_async_copy(strip, out.at[pl.ds(place, 32)], sem)
    copy.start()
    copy.wait()


def blend_kernel(slabs, out):
    count = slabs.shape[0] // 96
    for row in range(3):
        through = jnp.ones((8, LANES), jnp.float32)
        colour = [jnp.zeros((8, LANES), jnp.float32)] * 3
        for slab in range(count):
            base = slab * 96 + row * 32
            for channel in range(3):
                colour[channel] = colour[channel] + through * slabs[base + channel * 8 : base + channel * 8 + 8, :]
            through = through * slabs[base + 24 : base + 32, :]
        for channel, value in enumerate((*colour, 1.0 - through)):
            for tile in range(8):
                out[row, channel : channel + 1, tile * LANES : (tile + 1) * LANES] = value[tile : tile + 1, :]


def f32(*shape):
    return jax.ShapeDtypeStruct(shape, jnp.float32)


def cost(flops, size):
    return pl.CostEstimate(flops=flops, bytes_accessed=size, transcendentals=0)


def composited(field):
    planes, rows, width = field.shape
    depth = lax.axis_size("depth")
    strips = lax.axis_size("tile")
    chips = depth // 2
    tiles = width // LANES
    spacing = 3.0 / (planes * depth)

    outer_out = pl.pallas_call(
        fetch_kernel,
        out_shape=f32((OUTER_ROWS + 1) * tiles, LANES),
        in_specs=[pl.BlockSpec(memory_space=pltpu.HBM)],
        out_specs=VMEM,
        scratch_shapes=[pltpu.VMEM((1, tiles, PITCH, LANES), jnp.float32), pltpu.SemaphoreType.DMA((tiles,))],
        compiler_params=pltpu.CompilerParams(vmem_limit_bytes=4 << 20),
        cost_estimate=cost(1 << 10, 1 << 20),
        name="fetch",
    )(field)
    outer = lax.ppermute(
        outer_out,
        "depth",
        [(2 * k + 1, 2 * k + 2) for k in range(chips - 1)] + [(2 * k + 2, 2 * k + 1) for k in range(chips - 1)],
    )
    partner = lax.ppermute(field, "depth", [(i, i ^ 1) for i in range(depth)])

    own, own_sums = pl.pallas_call(
        functools.partial(own_kernel, spacing),
        out_shape=(f32(planes, tiles + 1, PITCH, LANES), f32(4, rows // 16, tiles * 8, LANES)),
        in_specs=[pl.BlockSpec(memory_space=pltpu.HBM)],
        out_specs=(VMEM, VMEM),
        scratch_shapes=[pltpu.SemaphoreType.DMA((tiles,))],
        compiler_params=pltpu.CompilerParams(vmem_limit_bytes=12 << 20),
        cost_estimate=cost(1 << 26, 1 << 21),
        name="own",
    )(field)

    lines = (2 * planes + 1) * tiles
    sent, edge, inner = pl.pallas_call(
        edge_kernel,
        out_shape=(f32(lines, LANES), f32(lines, LANES), f32(lines, LANES)),
        in_specs=[VMEM, VMEM, VMEM],
        out_specs=(VMEM, VMEM, VMEM),
        compiler_params=pltpu.CompilerParams(vmem_limit_bytes=4 << 20),
        cost_estimate=cost(1 << 20, 1 << 19),
        name="edges",
    )(own, partner, outer)
    place = lambda d, s: d * strips + s
    beside = lax.ppermute(
        sent,
        ("depth", "tile"),
        [(place(2 * k, t), place(2 * k, t + 1)) for k in range(chips) for t in range(strips - 1)]
        + [(place(2 * k + 1, t + 1), place(2 * k + 1, t)) for k in range(chips) for t in range(strips - 1)],
    )

    sums = []
    for group in range(2):
        sums.append(
            pl.pallas_call(
                functools.partial(partner_kernel, spacing, group),
                out_shape=f32(4, 3, tiles * 8, LANES),
                in_specs=[VMEM] * 3,
                out_specs=VMEM,
                scratch_shapes=[pltpu.VMEM((planes + 1, tiles + 1, PITCH, LANES), jnp.float32)],
                compiler_params=pltpu.CompilerParams(vmem_limit_bytes=12 << 20),
                cost_estimate=cost(1 << 25, 1 << 20),
            )(own, partner, own_sums)
        )
    most = pl.pallas_call(
        functools.partial(outer_kernel, spacing),
        out_shape=f32(chips * 96, LANES),
        in_specs=[VMEM] * 4,
        out_specs=VMEM,
        scratch_shapes=[pltpu.VMEM(((tiles + 1) * OUTER_ROWS, LANES), jnp.float32)],
        compiler_params=pltpu.CompilerParams(vmem_limit_bytes=12 << 20),
        cost_estimate=cost(1 << 24, 1 << 21),
        name="outer",
    )(*sums, own, outer)
    parts = pl.pallas_call(
        functools.partial(line_kernel, spacing),
        out_shape=f32(chips * 96, LANES),
        in_specs=[pl.BlockSpec(memory_space=pl.ANY)] + [VMEM] * 3,
        out_specs=pl.BlockSpec(memory_space=pl.ANY),
        input_output_aliases={0: 0},
        scratch_shapes=[pltpu.VMEM((32, LANES), jnp.float32), pltpu.SemaphoreType.DMA],
        compiler_params=pltpu.CompilerParams(vmem_limit_bytes=4 << 20),
        cost_estimate=cost(1 << 20, 1 << 18),
        name="line",
    )(most, edge, inner, beside)
    slabs = lax.all_to_all(
        parts.reshape(chips, 96, LANES),
        "depth",
        split_axis=0,
        concat_axis=0,
        tiled=True,
        axis_index_groups=[[2 * k + c for k in range(chips)] for c in range(2)],
    )
    image = pl.pallas_call(
        blend_kernel,
        out_shape=f32(3, 4, width),
        in_specs=[VMEM],
        out_specs=VMEM,
        compiler_params=pltpu.CompilerParams(vmem_limit_bytes=8 << 20),
        name="blend",
    )(slabs.reshape(chips * 96, LANES))
    return jnp.transpose(image, (1, 0, 2))


def solution(mesh):
    return jax.shard_map(
        composited,
        mesh=mesh,
        in_specs=(P("depth", "tile", None),),
        out_specs=P(None, ("tile", "depth"), None),
        check_vma=False,
    )
```
